8 devices in a mesh: data: 2 (over z, y), stage: 4 (over x, core).
Axes of the slice: x: 2, y: 2, z: 1, core: 2. Of those that a mesh axis runs over, the one named last changes fastest.
Arguments:
- X: bfloat16 [8, 1024, 2048], P('data'), parts along dimension 0
- G: bfloat16 [8, 1024, 2048], P('data'), parts along dimension 0
- W1: bfloat16 [4, 2048, 8192], P('stage')
- W2: bfloat16 [4, 8192, 2048], P('stage')
Outputs:
- output 1: bfloat16 [8, 1024, 2048], P('data'), parts along dimension 0
- output 2: bfloat16 [8, 1024, 2048], P('data'), parts along dimension 0
- output 3: float32 [8, 2048, 8192], P(('data', 'stage')), parts along dimension 0
- output 4: float32 [8, 8192, 2048], P(('data', 'stage')), parts along dimension 0
There are 2 independent parts. The reference program is written for one: setup_inputs(seed, part) draws one part's arguments, and reference() takes and returns one part's arrays. A program takes and returns all parts, laid end to end along the dimension named above; an argument that names none is the same for every part.
All inputs are finite; a program needn't handle non-finite values.
Results may differ from the reference program's by a relative error of at most 0.00996297.
Values are sent between devices in bfloat16 or wider.
A program may use at most 1 GiB of HBM per device.

```python
import jax
import jax.numpy as jnp
from jax import lax

D = 2048
F = 8192
LAYERS = 4
M = 4
B = 1024


def setup_inputs(seed: int = 0, part: int = 0) -> dict:
    key = jax.random.PRNGKey(seed)
    ks, kpb = jax.random.split(key)
    kp = jax.random.fold_in(kpb, part)
    kx, kg = jax.random.split(kp)
    k1, k2 = jax.random.split(ks)
    X = jax.random.normal(kx, (M, B, D), jnp.float32).astype(jnp.bfloat16)
    G = jax.random.normal(kg, (M, B, D), jnp.float32).astype(jnp.bfloat16)
    W1 = (jax.random.normal(k1, (LAYERS, D, F), jnp.float32) * D ** -0.5).astype(jnp.bfloat16)
    W2 = (jax.random.normal(k2, (LAYERS, F, D), jnp.float32) * (F * LAYERS) ** -0.5).astype(jnp.bfloat16)
    return {'X': X, 'G': G, 'W1': W1, 'W2': W2}


def _fwd_layer(h, w1, w2):
    z = jnp.dot(h, w1, preferred_element_type=jnp.float32)
    u = jax.nn.gelu(z, approximate=True).astype(jnp.bfloat16)
    return (h.astype(jnp.float32) + jnp.dot(u, w2, preferred_element_type=jnp.float32)).astype(jnp.bfloat16)


def _bwd_layer(h, g, w1, w2):
    z = jnp.dot(h, w1, preferred_element_type=jnp.float32)
    u, gelu_vjp = jax.vjp(lambda t: jax.nn.gelu(t, approximate=True), z)
    du = jnp.dot(g, w2.T, preferred_element_type=jnp.float32)
    dz = gelu_vjp(du)[0].astype(jnp.bfloat16)
    dw2 = jnp.dot(u.astype(jnp.bfloat16).T, g, preferred_element_type=jnp.float32)
    dw1 = jnp.dot(h.T, dz, preferred_element_type=jnp.float32)
    dh = (g.astype(jnp.float32) + jnp.dot(dz, w1.T, preferred_element_type=jnp.float32)).astype(jnp.bfloat16)
    return dh, dw1, dw2


def reference(X, G, W1, W2):
    def one(carry, xg):
        a1, a2 = carry
        x, g = xg

        def fstep(h, w):
            return _fwd_layer(h, w[0], w[1]), h
        y, hs = lax.scan(fstep, x, (W1, W2))

        def bstep(gh, inp):
            w1, w2, h, c1, c2 = inp
            dh, dw1, dw2 = _bwd_layer(h, gh, w1, w2)
            return dh, (c1 + dw1, c2 + dw2)
        dx, (a1, a2) = lax.scan(bstep, g, (W1, W2, hs, a1, a2), reverse=True)
        return (a1, a2), (y, dx)

    init = (jnp.zeros(W1.shape, jnp.float32), jnp.zeros(W2.shape, jnp.float32))
    (dW1, dW2), (Y, dX) = lax.scan(one, init, (X, G))
    return Y, dX, dW1, dW2
```

```python
import functools

import jax
import jax.numpy as jnp
from jax import lax
from jax.experimental import pallas as pl
from jax.experimental.pallas import tpu as pltpu
from jax.sharding import PartitionSpec as P

MESH = pl.DeviceIdType.MESH
C0 = 0.7978845608028654
C1 = 0.044715
CH = 256
HT = 1024
LAG = 4
F32 = jnp.float32
BF16 = jnp.bfloat16


def _nn(a, b):
    return lax.dot_general(a, b, (((1,), (0,)), ((), ())), preferred_element_type=F32)


def _nt(a, b):
    return lax.dot_general(a, b, (((1,), (1,)), ((), ())), preferred_element_type=F32)


def _gelu_parts(z):
    z2 = z * z
    t = jnp.tanh(z * (C0 + (C0 * C1) * z2))
    p = 0.5 + 0.5 * t
    gp = p + (z * (0.5 - 0.5 * (t * t))) * (C0 + (3.0 * C0 * C1) * z2)
    return (z * p).astype(BF16), gp


def _pipe_kernel(nc, n_b, x, g, w1, w2, y, dx, hin, gin, u, dz, gp,
                 w1p, w2p, w1s, w2s, acc, inb, outb, gpe, gpo, ue, uo,
                 pin_sem, w1_sem, w2_sem, in_sem, save_sem, oue, ouo, oge, ogo, ige, igo,
                 snd, snd_b, loc, fwd, recv_h, recv_g, recv_y, recv_dx):
    s = lax.axis_index('stage')
    first, last = s == 0, s == 3
    n_ops = nc + n_b
    warm = 8 - 2 * s - s // 3
    pairs = nc - warm

    def peer(j):
        return {'stage': j}

    def op_of(k):
        r = k - warm
        half = r // 2
        odd = r - 2 * half
        early = k < warm
        late = r >= 2 * pairs
        is_f = early | ((odd == 1) & (r < 2 * pairs))
        c = jnp.where(early, k, jnp.where(late, k - nc, jnp.where(odd == 1, warm + half, half)))
        return is_f, c

    def w1_copy(t, slot):
        return pltpu.make_async_copy(w1.at[:, pl.ds(pl.multiple_of(t * HT, HT), HT)], w1s.at[slot], w1_sem.at[slot])

    def w2_copy(t, slot):
        return pltpu.make_async_copy(w2.at[pl.ds(pl.multiple_of(t * HT, HT), HT), :], w2s.at[slot], w2_sem.at[slot])

    def pin_w1(i):
        return pltpu.make_async_copy(w1.at[:, pl.ds((2 * i + 1) * HT, HT)], w1p.at[i], pin_sem.at[i])

    def pin_w2(i):
        return pltpu.make_async_copy(w2.at[pl.ds(2 * i * HT, HT), :], w2p.at[i], pin_sem.at[4 + i])

    def hid(ref, c, t):
        return ref.at[pl.ds(pl.multiple_of(c * CH, CH), CH), pl.ds(pl.multiple_of(t * HT, HT), HT)]

    def remote(src, dst, send, recv, j):
        return pltpu.make_async_remote_copy(src_ref=src, dst_ref=dst, send_sem=send, recv_sem=recv,
                                            device_id=peer(j), device_id_type=MESH)

    def wait_recv(dst, recv):
        remote(outb.at[0], dst, snd.at[0], recv, 0).wait_recv()

    def fetch_input(k):
        is_f, c = op_of(k)
        slot = lax.rem(k, 2)

        @pl.when(is_f & first)
        def _():
            pltpu.make_async_copy(x.at[c], inb.at[slot], in_sem.at[slot]).start()

        @pl.when(is_f & (s > 0))
        def _():
            wait_recv(hin.at[c], recv_h.at[c])
            pltpu.make_async_copy(hin.at[c], inb.at[slot], in_sem.at[slot]).start()

        @pl.when((~is_f) & last)
        def _():
            pltpu.make_async_copy(g.at[c], inb.at[slot], in_sem.at[slot]).start()

        @pl.when((~is_f) & (s < 3))
        def _():
            wait_recv(gin.at[c], recv_g.at[c])
            pltpu.make_async_copy(gin.at[c], inb.at[slot], in_sem.at[slot]).start()

        @pl.when(~is_f)
        def _():
            pltpu.make_async_copy(gp.at[c, 0], gpe.at[1], ige.at[1]).start()

    def free_out(k):
        slot = lax.rem(k, 2)

        @pl.when(k >= 2)
        def _():
            was_f, c = op_of(k - 2)
            edge = (was_f & last) | ((~was_f) & first)
            remote(outb.at[slot], hin.at[0], snd.at[slot], recv_h.at[0], 0).wait_send()

            @pl.when(edge)
            def _():
                remote(outb.at[slot], hin.at[0], snd_b.at[slot], recv_h.at[0], 0).wait_send()
                pltpu.make_async_copy(outb.at[slot], y.at[0], loc.at[slot]).wait()

    def out_u(ref, c, t, buf, slot, sem):
        return pltpu.make_async_copy(buf.at[slot], hid(ref, c, t), sem.at[slot])

    def out_gp(c, t, buf, slot, sem):
        return pltpu.make_async_copy(buf.at[slot], gp.at[c, t], sem.at[slot])

    def forward(k, c):
        slot = lax.rem(k, 2)
        pltpu.make_async_copy(x.at[0], inb.at[slot], in_sem.at[slot]).wait()

        @pl.when(first)
        def _():
            pltpu.make_async_copy(inb.at[slot], hin.at[c], save_sem.at[slot]).start()

        w1_copy(0, 0).wait()
        acc[...] = inb[slot].astype(F32)
        ub, gpv = _gelu_parts(_nn(inb[slot], w1s[0]))
        ue[1] = ub
        gpe[1] = gpv
        out_u(u, c, 0, ue, 1, oue).start()
        out_gp(c, 0, gpe, 1, oge).start()

        def body(b, _):
            p, q = lax.rem(b, 2), 1 - lax.rem(b, 2)

            @pl.when(k == 0)
            def _():
                for i in range(3):
                    @pl.when(b == i)
                    def _():
                        pin_w2(i).wait()
                        pin_w1(i).wait()

            w2_copy(2 * b + 1, p).wait()
            w1_copy(2 * b + 2, q).wait()

            @pl.when(b >= 1)
            def _():
                out_u(u, c, 2 * b - 2, ue, p, oue).wait()
                out_gp(c, 2 * b - 2, gpe, p, oge).wait()
                w2_copy(2 * b + 3, q).start()

            @pl.when(b == 2)
            def _():
                out_u(u, c, 1, uo, 0, ouo).wait()
                out_gp(c, 1, gpo, 0, ogo).wait()

            w1_copy(lax.rem(2 * b + 4, 8), p).start()
            acc[...] += _nn(ue[q], w2p[b])
            ub, gpv = _gelu_parts(_nn(inb[slot], w1p[b]))
            uo[p] = ub
            gpo[p] = gpv
            out_u(u, c, 2 * b + 1, uo, p, ouo).start()
            out_gp(c, 2 * b + 1, gpo, p, ogo).start()
            ub, gpv = _gelu_parts(_nn(inb[slot], w1s[q]))
            ue[p] = ub
            gpe[p] = gpv
            out_u(u, c, 2 * b + 2, ue, p, oue).start()
            out_gp(c, 2 * b + 2, gpe, p, oge).start()
            acc[...] += _nn(uo[p], w2s[p])
            return 0

        lax.fori_loop(0, 3, body, 0)

        @pl.when(k == 0)
        def _():
            pin_w2(3).wait()
            pin_w1(3).wait()

        w2_copy(7, 1).wait()
        out_u(u, c, 3, uo, 1, ouo).wait()
        out_gp(c, 3, gpo, 1, ogo).wait()
        out_u(u, c, 4, ue, 1, oue).wait()
        out_gp(c, 4, gpe, 1, oge).wait()
        free_out(k)

        @pl.when(first)
        def _():
            pltpu.make_async_copy(inb.at[slot], hin.at[c], save_sem.at[slot]).wait()

        @pl.when(k + 1 < n_ops)
        def _():
            fetch_input(k + 1)

        w1_copy(2, 1).start()
        w2_copy(1, 0).start()
        ub, gpv = _gelu_parts(_nn(inb[slot], w1p[3]))
        uo[1] = ub
        gpo[1] = gpv
        out_u(u, c, 7, uo, 1, ouo).start()
        out_gp(c, 7, gpo, 1, ogo).start()
        acc[...] += _nn(ue[0], w2p[3])
        outb[slot] = (acc[...] + _nn(uo[1], w2s[1])).astype(BF16)
        w2_copy(3, 1).start()

        @pl.when(s < 3)
        def _():
            remote(outb.at[slot], hin.at[c], snd.at[slot], recv_h.at[c], s + 1).start()

        @pl.when(last)
        def _():
            remote(outb.at[slot], y.at[c], snd.at[slot], recv_y.at[c], 1).start()
            remote(outb.at[slot], y.at[c], snd_b.at[slot], recv_y.at[c], 2).start()
            pltpu.make_async_copy(outb.at[slot], y.at[c], loc.at[slot]).start()

        out_u(u, c, 5, uo, 0, ouo).wait()
        out_gp(c, 5, gpo, 0, ogo).wait()
        out_u(u, c, 6, ue, 0, oue).wait()
        out_gp(c, 6, gpe, 0, oge).wait()
        out_u(u, c, 7, uo, 1, ouo).wait()
        out_gp(c, 7, gpo, 1, ogo).wait()

    def pass_on_y(c):
        return remote(y.at[c], y.at[c], fwd.at[c], recv_y.at[c], 0)

    def pass_on_dx(c):
        return remote(dx.at[c], dx.at[c], fwd.at[c], recv_dx.at[c], 3)

    def in_gp(c, t, buf, slot, sem):
        return pltpu.make_async_copy(gp.at[c, t], buf.at[slot], sem.at[slot])

    def backward(k, c):
        slot = lax.rem(k, 2)
        in_gp(c, 1, gpo, 0, igo).start()
        in_gp(c, 2, gpe, 0, ige).start()

        @pl.when(s == 1)
        def _():
            wait_recv(y.at[c], recv_y.at[c])
            pass_on_y(c).start()

        @pl.when((s == 2) & (c >= LAG))
        def _():
            wait_recv(dx.at[c - LAG], recv_dx.at[c - LAG])
            pass_on_dx(c - LAG).start()

        pltpu.make_async_copy(x.at[0], inb.at[slot], in_sem.at[slot]).wait()

        @pl.when(last)
        def _():
            pltpu.make_async_copy(inb.at[slot], gin.at[c], save_sem.at[slot]).start()

        in_gp(c, 0, gpe, 1, ige).wait()
        acc[...] = inb[slot].astype(F32)
        ue[1] = (_nt(inb[slot], w2p[0]) * gpe[1]).astype(BF16)
        out_u(dz, c, 0, ue, 1, oue).start()

        def body(b, _):
            p, q = lax.rem(b, 2), 1 - lax.rem(b, 2)
            w1_copy(2 * b, p).wait()
            w2_copy(2 * b + 1, p).wait()
            in_gp(c, 2 * b + 1, gpo, p, igo).wait()
            in_gp(c, 2 * b + 2, gpe, p, ige).wait()

            @pl.when(b >= 1)
            def _():
                out_u(dz, c, 2 * b - 2, ue, p, oue).wait()
                w1_copy(2 * b + 2, q).start()
                w2_copy(2 * b + 3, q).start()

            @pl.when(b == 2)
            def _():
                out_u(dz, c, 1, uo, 0, ouo).wait()

            in_gp(c, 2 * b + 3, gpo, q, igo).start()

            @pl.when(b < 2)
            def _():
                in_gp(c, 2 * b + 4, gpe, q, ige).start()

            acc[...] += _nt(ue[q], w1s[p])
            uo[p] = (_nt(inb[slot], w2s[p]) * gpo[p]).astype(BF16)
            out_u(dz, c, 2 * b + 1, uo, p, ouo).start()
            ue[p] = (_nt(inb[slot], w2p[b + 1]) * gpe[p]).astype(BF16)
            out_u(dz, c, 2 * b + 2, ue, p, oue).start()
            acc[...] += _nt(uo[p], w1p[b])
            return 0

        lax.fori_loop(0, 3, body, 0)
        w1_copy(6, 1).wait()
        w2_copy(7, 1).wait()
        in_gp(c, 7, gpo, 1, igo).wait()
        out_u(dz, c, 3, uo, 1, ouo).wait()
        out_u(dz, c, 4, ue, 1, oue).wait()
        free_out(k)

        @pl.when(last)
        def _():
            pltpu.make_async_copy(inb.at[slot], gin.at[c], save_sem.at[slot]).wait()

        @pl.when(k + 1 < n_ops)
        def _():
            fetch_input(k + 1)

        w1_copy(0, 0).start()
        w2_copy(1, 0).start()
        uo[1] = (_nt(inb[slot], w2s[1]) * gpo[1]).astype(BF16)
        out_u(dz, c, 7, uo, 1, ouo).start()
        acc[...] += _nt(ue[0], w1s[1])
        outb[slot] = (acc[...] + _nt(uo[1], w1p[3])).astype(BF16)
        w1_copy(2, 1).start()
        w2_copy(3, 1).start()

        @pl.when(s > 0)
        def _():
            remote(outb.at[slot], gin.at[c], snd.at[slot], recv_g.at[c], s - 1).start()

        @pl.when(first)
        def _():
            remote(outb.at[slot], dx.at[c], snd.at[slot], recv_dx.at[c], 2).start()
            remote(outb.at[slot], dx.at[c], snd_b.at[slot], recv_dx.at[c], 1).start()
            pltpu.make_async_copy(outb.at[slot], dx.at[c], loc.at[slot]).start()

        out_u(dz, c, 5, uo, 0, ouo).wait()
        out_u(dz, c, 6, ue, 0, oue).wait()
        out_u(dz, c, 7, uo, 1, ouo).wait()

    w1_copy(0, 0).start()
    for i in range(4):
        pin_w2(i).start()
        pin_w1(i).start()
        if i == 0:
            w2_copy(1, 0).start()
            w1_copy(2, 1).start()
        if i == 1:
            w2_copy(3, 1).start()
    barrier = pltpu.get_barrier_semaphore()
    for d in range(1, 4):
        pl.semaphore_signal(barrier, inc=1, device_id=peer(lax.rem(s + d, 4)), device_id_type=MESH)
    pl.semaphore_wait(barrier, 3)
    fetch_input(0)

    def step(k, _):
        is_f, c = op_of(k)

        @pl.when(is_f)
        def _():
            forward(k, c)

        @pl.when(~is_f)
        def _():
            backward(k, c)

        return 0

    lax.fori_loop(0, n_ops, step, 0)

    w1_copy(0, 0).wait()
    w1_copy(2, 1).wait()
    w2_copy(1, 0).wait()
    w2_copy(3, 1).wait()
    free_out(n_ops)
    free_out(n_ops + 1)

    def tail(c, _):
        @pl.when((s == 2) & (c >= n_b - LAG))
        def _():
            wait_recv(dx.at[c], recv_dx.at[c])
            pass_on_dx(c).start()

        @pl.when((s == 1) | (s == 3))
        def _():
            wait_recv(dx.at[c], recv_dx.at[c])

        @pl.when((s == 0) | (s == 2))
        def _():
            wait_recv(y.at[c], recv_y.at[c])

        return 0

    lax.fori_loop(0, nc, tail, 0)

    def drain(c, _):
        @pl.when(s == 1)
        def _():
            pass_on_y(c).wait_send()

        @pl.when(s == 2)
        def _():
            pass_on_dx(c).wait_send()

        return 0

    lax.fori_loop(0, nc, drain, 0)


def _pipe(x, g, w1, w2):
    tokens, d = x.shape
    h = w1.shape[1]
    nc, nt = tokens // CH, h // HT
    rows = jax.ShapeDtypeStruct((nc, CH, d), BF16)
    wide = jax.ShapeDtypeStruct((tokens, h), BF16)
    anyspec = pl.BlockSpec(memory_space=pl.ANY)
    dma = pltpu.SemaphoreType.DMA
    outs = pl.pallas_call(
        functools.partial(_pipe_kernel, nc, nc),
        out_shape=(rows, rows, rows, rows, wide, wide, jax.ShapeDtypeStruct((nc, nt, CH, HT), F32)),
        in_specs=[anyspec] * 4,
        out_specs=(anyspec,) * 7,
        scratch_shapes=[
            pltpu.VMEM((4, d, HT), BF16), pltpu.VMEM((4, HT, d), BF16),
            pltpu.VMEM((2, d, HT), BF16), pltpu.VMEM((2, HT, d), BF16),
            pltpu.VMEM((CH, d), F32), pltpu.VMEM((2, CH, d), BF16), pltpu.VMEM((2, CH, d), BF16),
            pltpu.VMEM((2, CH, HT), F32), pltpu.VMEM((2, CH, HT), F32),
            pltpu.VMEM((2, CH, HT), BF16), pltpu.VMEM((2, CH, HT), BF16),
            dma((8,)), dma((2,)), dma((2,)), dma((2,)), dma((2,)), dma((2,)), dma((2,)), dma((2,)), dma((2,)), dma((2,)), dma((2,)),
            dma((2,)), dma((2,)), dma((2,)), dma((nc,)), dma((nc,)), dma((nc,)), dma((nc,)), dma((nc,)),
        ],
        compiler_params=pltpu.CompilerParams(collective_id=0, has_side_effects=True, vmem_limit_bytes=67043328),
        cost_estimate=pl.CostEstimate(flops=8 * tokens * d * h, bytes_accessed=2 << 30, transcendentals=tokens * h),
        name='pipe',
    )(x.reshape(nc, CH, d), g.reshape(nc, CH, d), w1, w2)
    return outs


def solution(mesh):
    def body(x, g, w1, w2):
        n_mb, mb, d = x.shape
        y, dx, hin, gin, u, dz, _ = _pipe(x.reshape(n_mb * mb, d), g.reshape(n_mb * mb, d), w1[0], w2[0])
        hin, gin = hin.reshape(n_mb * mb, d), gin.reshape(n_mb * mb, d)
        dw2 = jnp.dot(u.T, gin, preferred_element_type=F32)
        dw1 = jnp.dot(hin.T, dz, preferred_element_type=F32)
        return y.reshape(x.shape), dx.reshape(x.shape), dw1[None], dw2[None]

    return jax.shard_map(body, mesh=mesh,
                         in_specs=(P('data'), P('data'), P('stage'), P('stage')),
                         out_specs=(P('data'), P('data'), P(('data', 'stage')), P(('data', 'stage'))),
                         check_vma=False)
```

```python
import functools

import jax
import jax.numpy as jnp
from jax import lax
from jax.experimental import pallas as pl
from jax.experimental.pallas import tpu as pltpu
from jax.sharding import PartitionSpec as P

MESH = pl.DeviceIdType.MESH
C0 = 0.7978845608028654
C1 = 0.044715
CH = 256
HT = 1024
DX_OP = 18
Y_FIRST = 12
Y_BLOCK = 3
EARLY = (8, 6, 2, 0)
VMEM_MAX = 67043328
F32 = jnp.float32
BF16 = jnp.bfloat16


def _nn(a, b):
    return lax.dot_general(a, b, (((1,), (0,)), ((), ())), preferred_element_type=F32)


def _nt(a, b):
    return lax.dot_general(a, b, (((1,), (1,)), ((), ())), preferred_element_type=F32)


def _tn(a, b):
    return lax.dot_general(a, b, (((0,), (0,)), ((), ())), preferred_element_type=F32)


def _gelu_parts(z):
    z2 = z * z
    p = jax.nn.sigmoid(z * (2.0 * C0 + (2.0 * C0 * C1) * z2))
    gu = z * p
    gp = p + (gu * (1.0 - p)) * (2.0 * C0 + (6.0 * C0 * C1) * z2)
    return gu.astype(BF16), gp


def _pipe_kernel(n_f, b0, n_b, *refs):
    if n_f:
        x, g, w1, w2, y, dx, hin, gin, u, dz, gp = refs[:11]
        part = None
        scratch = refs[11:]
    else:
        g, w1, w2, gp, u, _, _, _, _, _, y, dx, gin, dz, part = refs[:15]
        x = hin = None
        scratch = refs[15:]
    fwd, recv_y, recv_dx, more = scratch[15:19]
    _chunks(n_f, b0, n_b, x, g, w1, w2, y, dx, hin, gin, u, dz, gp, part, *scratch)
    s = lax.axis_index('stage')
    row, remote, wait_recv = _moves()
    n_ops = n_f + n_b
    dx_from = (n_ops - DX_OP + 1) // 2 if n_f else 0
    y0, n_y = (0, Y_FIRST) if n_f else (Y_FIRST, (b0 + n_b) - Y_FIRST)
    y_from = n_b if n_f else 0

    def tail_y(j, _):
        c = y0 + j

        @pl.when((s == 1) & (j >= y_from))
        def _():
            wait_recv(row(y, c), recv_y.at[j])
            remote(row(y, c), row(y, c), fwd.at[j], recv_y.at[j], 0).start()

        @pl.when((s == 0) | (s == 2))
        def _():
            wait_recv(row(y, c), recv_y.at[j])

        return 0

    def tail_dx(j, _):
        c = b0 + j

        @pl.when((s == 2) & (j >= dx_from))
        def _():
            wait_recv(row(dx, c), recv_dx.at[j])
            remote(row(dx, c), row(dx, c), fwd.at[j], recv_dx.at[j], 3).start()

        @pl.when((s == 1) | (s == 3))
        def _():
            wait_recv(row(dx, c), recv_dx.at[j])

        return 0

    lax.fori_loop(0, n_y, tail_y, 0)
    lax.fori_loop(0, n_b, tail_dx, 0)

    def drain(j, _):
        @pl.when(((s == 1) & (j < n_y)) | ((s == 2) & (j < n_b)))
        def _():
            remote(row(y, 0), row(y, 0), fwd.at[j], recv_y.at[j], 0).wait_send()

        if not n_f:
            @pl.when((s == 3) & (j < n_y))
            def _():
                remote(row(y, 0), row(y, 0), fwd.at[j], recv_y.at[j], 0).wait_send()
                remote(row(y, 0), row(y, 0), more.at[j], recv_y.at[j], 0).wait_send()

        return 0

    lax.fori_loop(0, max(n_y, n_b), drain, 0)


def _moves():
    def row(ref, c):
        return ref.at[pl.ds(pl.multiple_of(c * CH, CH), CH), :]

    def remote(src, dst, send, recv, j):
        return pltpu.make_async_remote_copy(src_ref=src, dst_ref=dst, send_sem=send, recv_sem=recv,
                                            device_id={'stage': j}, device_id_type=MESH)

    def wait_recv(dst, recv):
        remote(dst, dst, recv, recv, 0).wait_recv()

    return row, remote, wait_recv


def _per_stage(s, counts):
    return sum(jnp.where(s == i, c, 0) for i, c in enumerate(counts))


def _chunks(n_f, b0, n_b, x, g, w1, w2, y, dx, hin, gin, u, dz, gp, part,
            pin_sem, w1_sem, w2_sem, in_sem, save_sem, oue, ouo, oge, ogo, ige, igo,
            snd, snd_b, loc, recv_g, fwd, recv_y, recv_dx, more,
            w1p, w2p, w1s, w2s, acc, inb, outb, gpe, gpo, ue, uo):
    recv_h = more
    row, remote, wait_recv = _moves()
    s = lax.axis_index('stage')
    first, last = s == 0, s == 3
    n_ops = n_f + n_b
    if n_f:
        warm = 16 - 4 * s - 4 * (s // 2) + (s // 3)
        pairs = jnp.minimum(n_b, n_f - warm)

    def peer(j):
        return {'stage': j}

    def op_of(k):
        if not n_f:
            return False, b0 + k
        r = k - warm
        half = r // 2
        odd = r - 2 * half
        early = k < warm
        late = r >= 2 * pairs
        late_f = warm + pairs < n_f
        is_f = early | ((odd == 1) & (~late)) | (late & late_f)
        c_late = jnp.where(late_f, warm + pairs, pairs) + r - 2 * pairs
        c = jnp.where(early, k, jnp.where(late, c_late, jnp.where(odd == 1, warm + half, half)))
        return is_f, c

    def w1_copy(t, slot):
        return pltpu.make_async_copy(w1.at[:, pl.ds(pl.multiple_of(t * HT, HT), HT)], w1s.at[slot], w1_sem.at[slot])

    def w2_copy(t, slot):
        return pltpu.make_async_copy(w2.at[pl.ds(pl.multiple_of(t * HT, HT), HT), :], w2s.at[slot], w2_sem.at[slot])

    def pin_w1(i):
        return pltpu.make_async_copy(w1.at[:, pl.ds((2 * i + 1) * HT, HT)], w1p.at[i], pin_sem.at[i])

    def pin_w2(i):
        return pltpu.make_async_copy(w2.at[pl.ds(2 * i * HT, HT), :], w2p.at[i], pin_sem.at[4 + i])

    def wait_pins(k, b):
        @pl.when(k == 0)
        def _():
            for i in range(3):
                @pl.when(b == i)
                def _():
                    pin_w2(i if n_f else i + 1).wait()
                    pin_w1(i).wait()

    def hid(ref, c, t):
        return ref.at[pl.ds(pl.multiple_of(c * CH, CH), CH), pl.ds(pl.multiple_of(t * HT, HT), HT)]

    def load_input(ref, c, slot):
        return pltpu.make_async_copy(row(ref, c), inb.at[slot], in_sem.at[slot])

    def fetch_input(k):
        is_f, c = op_of(k)
        slot = lax.rem(k, 2)
        is_b = True if not n_f else ~is_f
        if n_f:
            @pl.when(is_f & first)
            def _():
                load_input(x, c, slot).start()

            @pl.when(is_f & (s > 0))
            def _():
                wait_recv(row(hin, c), recv_h.at[c])
                load_input(hin, c, slot).start()

        @pl.when(is_b & last)
        def _():
            load_input(g, c, slot).start()

        @pl.when(is_b & (s < 3))
        def _():
            wait_recv(row(gin, c), recv_g.at[c])
            load_input(gin, c, slot).start()

        @pl.when(is_b)
        def _():
            in_gp(c, 0, *place(0)).start()

    def exits(k):
        is_f, c = op_of(k)
        if not n_f:
            return True, first, first
        share = (is_f & last & (c < Y_FIRST)) | ((~is_f) & first)
        own = (is_f & last) | ((~is_f) & first)
        return share | (~own), share, own

    def free_out(k):
        slot = lax.rem(k, 2)

        @pl.when(k >= 2)
        def _():
            one, two, own = exits(k - 2)

            @pl.when(one)
            def _():
                remote(outb.at[slot], row(gin, 0), snd.at[slot], recv_g.at[0], 0).wait_send()

            @pl.when(two)
            def _():
                remote(outb.at[slot], row(gin, 0), snd_b.at[slot], recv_g.at[0], 0).wait_send()

            @pl.when(own)
            def _():
                pltpu.make_async_copy(outb.at[slot], row(dx, 0), loc.at[slot]).wait()

    def place(t):
        return t % 2, (t - 1) // 2 % 2

    def out_u(ref, c, t, odd, slot):
        return pltpu.make_async_copy((ue, uo)[odd].at[slot], hid(ref, c, t), (oue, ouo)[odd].at[slot])

    def out_gp(c, t, odd, slot):
        return pltpu.make_async_copy((gpe, gpo)[odd].at[slot], gp.at[c, t], (oge, ogo)[odd].at[slot])

    def in_gp(c, t, odd, slot):
        return pltpu.make_async_copy(gp.at[c, t], (gpe, gpo)[odd].at[slot], (ige, igo)[odd].at[slot])

    def flush(ref, c, *tiles):
        for t in tiles:
            out_u(ref, c, t, *place(t)).wait()
            if ref is not dz:
                out_gp(c, t, *place(t)).wait()

    def emit(c, t, odd, slot):
        out_u(u, c, t, odd, slot).start()
        out_gp(c, t, odd, slot).start()

    def forward(k, c):
        slot = lax.rem(k, 2)
        load_input(x, 0, slot).wait()

        @pl.when(first)
        def _():
            pltpu.make_async_copy(inb.at[slot], row(hin, c), save_sem.at[slot]).start()

        w1_copy(0, 0).wait()
        acc[...] = inb[slot].astype(F32)
        ub, gpv = _gelu_parts(_nn(inb[slot], w1s[0]))
        ue[1] = ub
        gpe[1] = gpv
        emit(c, 0, *place(0))

        def body(b, _):
            p, q = lax.rem(b, 2), 1 - lax.rem(b, 2)
            wait_pins(k, b)
            w2_copy(2 * b + 1, p).wait()
            w1_copy(2 * b + 2, q).wait()

            @pl.when(b >= 1)
            def _():
                out_u(u, c, 2 * b - 2, 0, p).wait()
                out_gp(c, 2 * b - 2, 0, p).wait()
                w2_copy(2 * b + 3, q).start()

            @pl.when(b == 2)
            def _():
                flush(u, c, 1)

            w1_copy(lax.rem(2 * b + 4, 8), p).start()
            acc[...] += _nn(ue[q], w2p[b])
            ub, gpv = _gelu_parts(_nn(inb[slot], w1p[b]))
            uo[p] = ub
            gpo[p] = gpv
            ub, gpv = _gelu_parts(_nn(inb[slot], w1s[q]))
            ue[p] = ub
            gpe[p] = gpv
            acc[...] += _nn(uo[p], w2s[p])
            emit(c, 2 * b + 1, 1, p)
            emit(c, 2 * b + 2, 0, p)
            return 0

        lax.fori_loop(0, 3, body, 0)

        @pl.when(k == 0)
        def _():
            pin_w2(3).wait()
            pin_w1(3).wait()

        w2_copy(7, 1).wait()
        flush(u, c, 3, 4)
        free_out(k)

        @pl.when(first)
        def _():
            pltpu.make_async_copy(inb.at[slot], row(hin, c), save_sem.at[slot]).wait()

        @pl.when((k > 0) & (k + 1 < n_ops) & (k + 1 != warm))
        def _():
            fetch_input(k + 1)

        w2_copy(1, 0).start()
        w1_copy(2, 1).start()
        ub, gpv = _gelu_parts(_nn(inb[slot], w1p[3]))
        uo[1] = ub
        gpo[1] = gpv
        emit(c, 7, *place(7))
        acc[...] += _nn(ue[0], w2p[3])
        outb[slot] = (acc[...] + _nn(uo[1], w2s[1])).astype(BF16)

        @pl.when(s < 3)
        def _():
            remote(outb.at[slot], row(hin, c), snd.at[slot], recv_h.at[c], s + 1).start()

        @pl.when(last)
        def _():
            pltpu.make_async_copy(outb.at[slot], row(y, c), loc.at[slot]).start()

            @pl.when(c < Y_FIRST)
            def _():
                remote(outb.at[slot], row(y, c), snd.at[slot], recv_y.at[c], 1).start()
                remote(outb.at[slot], row(y, c), snd_b.at[slot], recv_y.at[c], 2).start()

        flush(u, c, 5, 6, 7)

        @pl.when((k == 0) | (k + 1 == warm))
        def _():
            fetch_input(k + 1)

        first_gp(k + 1)
        w2_copy(3, 1).start()

    def first_gp(k):
        is_f, c = op_of(k)

        @pl.when((k < n_ops) & (True if not n_f else ~is_f))
        def _():
            for t in (1, 2):
                in_gp(c, t, *place(t)).start()

    def pass_on_y(c):
        wait_recv(row(y, c), recv_y.at[c])
        remote(row(y, c), row(y, c), fwd.at[c], recv_y.at[c], 0).start()

    def backward(k, c):
        slot = lax.rem(k, 2)
        if n_f:
            @pl.when(s == 1)
            def _():
                pass_on_y(c)
        load_input(g, 0, slot).wait()

        @pl.when(last)
        def _():
            pltpu.make_async_copy(inb.at[slot], row(gin, c), save_sem.at[slot]).start()

        in_gp(c, 0, *place(0)).wait()
        if not n_f:
            @pl.when(k == 0)
            def _():
                pin_w2(0).wait()
        acc[...] = inb[slot].astype(F32)
        ue[1] = (_nt(inb[slot], w2p[0]) * gpe[1]).astype(BF16)
        out_u(dz, c, 0, *place(0)).start()

        def body(b, _):
            p, q = lax.rem(b, 2), 1 - lax.rem(b, 2)
            if not n_f:
                wait_pins(k, b)
            w1_copy(2 * b, p).wait()
            w2_copy(2 * b + 1, p).wait()
            in_gp(c, 2 * b + 1, 1, p).wait()
            in_gp(c, 2 * b + 2, 0, p).wait()

            @pl.when(b >= 1)
            def _():
                out_u(dz, c, 2 * b - 2, 0, p).wait()

            @pl.when(b == 2)
            def _():
                flush(dz, c, 1)

            in_gp(c, 2 * b + 3, 1, q).start()

            @pl.when(b < 2)
            def _():
                in_gp(c, 2 * b + 4, 0, q).start()

            @pl.when(b >= 1)
            def _():
                w1_copy(2 * b + 2, q).start()
                w2_copy(2 * b + 3, q).start()

            acc[...] += _nt(ue[q], w1s[p])
            uo[p] = (_nt(inb[slot], w2s[p]) * gpo[p]).astype(BF16)
            out_u(dz, c, 2 * b + 1, 1, p).start()
            ue[p] = (_nt(inb[slot], w2p[b + 1]) * gpe[p]).astype(BF16)
            out_u(dz, c, 2 * b + 2, 0, p).start()
            acc[...] += _nt(uo[p], w1p[b])
            return 0

        lax.fori_loop(0, 3, body, 0)
        if not n_f:
            @pl.when(k == 0)
            def _():
                pin_w1(3).wait()
        w1_copy(6, 1).wait()
        w2_copy(7, 1).wait()
        in_gp(c, 7, *place(7)).wait()
        flush(dz, c, 3, 4)
        free_out(k)

        @pl.when(last)
        def _():
            pltpu.make_async_copy(inb.at[slot], row(gin, c), save_sem.at[slot]).wait()

        @pl.when(k + 1 < n_ops)
        def _():
            fetch_input(k + 1)

        w1_copy(0, 0).start()
        w2_copy(1, 0).start()
        uo[1] = (_nt(inb[slot], w2s[1]) * gpo[1]).astype(BF16)
        out_u(dz, c, 7, *place(7)).start()
        acc[...] += _nt(ue[0], w1s[1])
        outb[slot] = (acc[...] + _nt(uo[1], w1p[3])).astype(BF16)
        if not n_f:
            @pl.when(k == 0)
            def _():
                pl.semaphore_wait(barrier, 2 - (s == 1).astype(jnp.int32))

        @pl.when(s > 0)
        def _():
            remote(outb.at[slot], row(gin, c), snd.at[slot], recv_g.at[c], s - 1).start()

        @pl.when(first)
        def _():
            pltpu.make_async_copy(outb.at[slot], row(dx, c), loc.at[slot]).start()
            remote(outb.at[slot], row(dx, c), snd.at[slot], recv_dx.at[c - b0], 2).start()
            remote(outb.at[slot], row(dx, c), snd_b.at[slot], recv_dx.at[c - b0], 1).start()

        first_gp(k + 1)
        w1_copy(2, 1).start()
        w2_copy(3, 1).start()
        flush(dz, c, 5, 6, 7)

    def half_blocks(lo, hi):
        half = w1p.shape[1]

        def g_copy(i):
            return pltpu.make_async_copy(gin.at[pl.ds(0, half), pl.ds(i * HT, HT)], w1p.at[i], pin_sem.at[i])

        def u_copy(i, slot):
            return pltpu.make_async_copy(u.at[pl.ds(0, half), pl.ds(pl.multiple_of(i * HT, HT), HT)], w1s.at[slot], w1_sem.at[slot])

        def out(i, j, p, buf, col, sem):
            rows = pl.ds(pl.multiple_of(i * HT + j * CH, CH), CH)
            return pltpu.make_async_copy(buf.at[p], part.at[rows, pl.ds(col * HT, HT)], sem.at[p])

        @pl.when(lo < hi)
        def _():
            u_copy(lo, 0).start()
            g_copy(0).start()
            g_copy(1).start()
            g_copy(0).wait()
            g_copy(1).wait()

            def block(i, _):
                slot = lax.rem(i - lo, 2)

                @pl.when(i + 1 < hi)
                def _():
                    u_copy(i + 1, 1 - slot).start()

                u_copy(i, slot).wait()

                @pl.when(last & (i == lo + Y_BLOCK))
                def _():
                    for j in range(b0 + n_b - Y_FIRST):
                        yj = row(y, Y_FIRST + j)
                        remote(yj, yj, fwd.at[j], recv_y.at[j], 1).start()
                        remote(yj, yj, more.at[j], recv_y.at[j], 2).start()

                def strips(jj, _):
                    @pl.when((i > lo) | (jj > 0))
                    def _():
                        for p in range(2):
                            out(i, 0, p, gpe, 0, oge).wait()
                            out(i, 0, p, gpo, 1, ogo).wait()

                    for p in range(2):
                        inb[p] = w1s[slot, :, pl.ds(pl.multiple_of((2 * jj + p) * CH, CH), CH)].T
                    for p in range(2):
                        gpe[p] = _nn(inb[p], w1p[0])
                        gpo[p] = _nn(inb[p], w1p[1])
                        out(i, 2 * jj + p, p, gpe, 0, oge).start()
                        out(i, 2 * jj + p, p, gpo, 1, ogo).start()
                    return 0

                lax.fori_loop(0, HT // CH // 2, strips, 0)
                return 0

            lax.fori_loop(lo, hi, block, 0)
            for p in range(2):
                out(lo, 0, p, gpe, 0, oge).wait()
                out(lo, 0, p, gpo, 1, ogo).wait()

    barrier = pltpu.get_barrier_semaphore()
    if n_f:
        @pl.when(first)
        def _():
            fetch_input(0)
        w1_copy(0, 0).start()
        for i in range(4):
            pin_w2(i).start()
            pin_w1(i).start()
            if i == 0:
                w2_copy(1, 0).start()
                w1_copy(2, 1).start()
            if i == 1:
                w2_copy(3, 1).start()
        for d in range(1, 4):
            pl.semaphore_signal(barrier, inc=1, device_id=peer(lax.rem(s + d, 4)), device_id_type=MESH)
        pl.semaphore_wait(barrier, 3)

        @pl.when(s > 0)
        def _():
            fetch_input(0)
    else:
        for to, frm in ((1, 0), (2, 1), (3, 1), (0, 1), (3, 2), (0, 2), (2, 3)):
            @pl.when(s == frm)
            def _():
                pl.semaphore_signal(barrier, inc=1, device_id=peer(to), device_id_type=MESH)
        @pl.when(last)
        def _():
            fetch_input(0)
        pin_w2(0).start()
        w1_copy(0, 0).start()
        w2_copy(1, 0).start()
        pin_w1(0).start()
        pin_w2(1).start()
        first_gp(0)
        w1_copy(2, 1).start()
        w2_copy(3, 1).start()
        for i in range(1, 4):
            pin_w1(i).start()
            if i < 3:
                pin_w2(i + 1).start()

        @pl.when(s < 3)
        def _():
            fetch_input(0)

    def step(k, _):
        is_f, c = op_of(k)
        if not n_f:
            backward(k, c)
            return 0
        gone = k - DX_OP
        cd = gone // 2

        @pl.when((s == 2) & (gone >= 0) & (gone == 2 * cd) & (gone < 2 * n_b))
        def _():
            wait_recv(row(dx, cd), recv_dx.at[cd])
            remote(row(dx, cd), row(dx, cd), fwd.at[cd], recv_dx.at[cd], 3).start()

        @pl.when(is_f)
        def _():
            forward(k, c)

        @pl.when(~is_f)
        def _():
            backward(k, c)

        return 0

    lax.fori_loop(0, n_ops, step, 0)

    w1_copy(0, 0).wait()
    w1_copy(2, 1).wait()
    w2_copy(1, 0).wait()
    w2_copy(3, 1).wait()
    free_out(n_ops)
    free_out(n_ops + 1)
    if not n_f:
        half_blocks(_per_stage(s, EARLY), u.shape[1] // HT)


def _scratch(nc, n_b, d, n_f):
    dma = pltpu.SemaphoreType.DMA
    sems = [dma((8,)), *[dma((2,))] * 13, *[dma((nc,))] * 5]
    return sems + [
        pltpu.VMEM((4, d, HT), BF16), pltpu.VMEM((4, HT, d), BF16),
        pltpu.VMEM((2, d, HT), BF16), pltpu.VMEM((2, HT, d), BF16),
        pltpu.VMEM((CH, d), F32), pltpu.VMEM((2, CH, d), BF16), pltpu.VMEM((2, CH, d), BF16),
        pltpu.VMEM((2, CH, HT), F32), pltpu.VMEM((2, CH, HT), F32),
        pltpu.VMEM((2, CH, HT), BF16), pltpu.VMEM((2, CH, HT), BF16)]


def _first_kernel(x, g, w1, w2, n_b):
    tokens, d = x.shape
    h = w1.shape[1]
    nc = tokens // CH
    rows = jax.ShapeDtypeStruct((tokens, d), BF16)
    wide = jax.ShapeDtypeStruct((tokens, h), BF16)
    anyspec = pl.BlockSpec(memory_space=pl.ANY)
    return pl.pallas_call(
        functools.partial(_pipe_kernel, nc, 0, n_b),
        out_shape=(rows, rows, rows, rows, wide, wide, jax.ShapeDtypeStruct((nc, h // HT, CH, HT), F32)),
        in_specs=[anyspec] * 4,
        out_specs=(anyspec,) * 7,
        scratch_shapes=_scratch(nc, n_b, d, nc),
        compiler_params=pltpu.CompilerParams(collective_id=0, has_side_effects=True, vmem_limit_bytes=VMEM_MAX),
        cost_estimate=pl.CostEstimate(flops=4 * (nc + n_b) * CH * d * h, bytes_accessed=1 << 30, transcendentals=0),
        name='pipe_a',
    )(x, g, w1, w2)


def _second_kernel(g, w1, w2, gp, u, y, dx, gin, dz, part, b0):
    tokens, d = g.shape
    h = w1.shape[1]
    nc = tokens // CH
    n_b = nc - b0
    anyspec = pl.BlockSpec(memory_space=pl.ANY)
    return pl.pallas_call(
        functools.partial(_pipe_kernel, 0, b0, n_b),
        out_shape=tuple(jax.ShapeDtypeStruct(a.shape, a.dtype) for a in (y, dx, gin, dz, part)),
        in_specs=[anyspec] * 10,
        out_specs=(anyspec,) * 5,
        scratch_shapes=_scratch(nc, n_b, d, 0),
        input_output_aliases={5 + i: i for i in range(5)},
        compiler_params=pltpu.CompilerParams(collective_id=1, has_side_effects=True, vmem_limit_bytes=VMEM_MAX),
        cost_estimate=pl.CostEstimate(flops=4 * n_b * CH * d * h, bytes_accessed=1 << 29, transcendentals=0),
        name='pipe_b',
    )(g, w1, w2, gp, u, y, dx, gin, dz, part)


def _half_blocks(lo, n, half, u, g, o):
    def block(u_ref, g_ref, o_ref):
        o_ref[...] = _tn(u_ref[...], g_ref[...])

    d = g.shape[1]
    pltpu.emit_pipeline(
        block, grid=(n,),
        in_specs=[pl.BlockSpec((half, 1024), lambda i: (0, lo + i)), pl.BlockSpec((half, d), lambda i: (0, 0))],
        out_specs=[pl.BlockSpec((1024, d), lambda i: (lo + i, 0))])(u, g, o)


def _early_kernel(half, u, g, o):
    n = _per_stage(lax.axis_index('stage'), EARLY)

    @pl.when(n > 0)
    def _():
        _half_blocks(0, n, half, u, g, o)


def _early_dw2(u, gin, half):
    tokens, h = u.shape
    d = gin.shape[1]
    anyspec = pl.BlockSpec(memory_space=pl.ANY)
    return pl.pallas_call(
        functools.partial(_early_kernel, half),
        in_specs=[anyspec] * 2,
        out_specs=anyspec,
        out_shape=jax.ShapeDtypeStruct((h, d), F32),
        compiler_params=pltpu.CompilerParams(vmem_limit_bytes=VMEM_MAX),
        cost_estimate=pl.CostEstimate(flops=half * d * h, bytes_accessed=1 << 26, transcendentals=0),
        name='early_dw2',
    )(u, gin)


def _dw2_kernel(u_ref, g_ref, part_ref, y_ref, o_ref, yo_ref):
    yo_ref[...] = y_ref[...]
    o_ref[...] = part_ref[...] + _tn(u_ref[...], g_ref[...])


def _dw2(u, gin, part, y, half):
    tokens, h = u.shape
    d = gin.shape[1]
    steps = h // 1024
    rows = pl.BlockSpec((tokens // steps, d), lambda i: (i, 0))
    blocks = pl.BlockSpec((1024, d), lambda i: (i, 0))
    return pl.pallas_call(
        _dw2_kernel,
        grid=(steps,),
        in_specs=[pl.BlockSpec((half, 1024), lambda i: (1, i)),
                  pl.BlockSpec((half, d), lambda i: (1, 0), pipeline_mode=pl.Buffered(1)), blocks, rows],
        out_specs=(blocks, rows),
        out_shape=(jax.ShapeDtypeStruct((h, d), F32), jax.ShapeDtypeStruct(y.shape, BF16)),
        compiler_params=pltpu.CompilerParams(vmem_limit_bytes=VMEM_MAX, dimension_semantics=('arbitrary',)),
        cost_estimate=pl.CostEstimate(flops=tokens * d * h, bytes_accessed=1 << 27, transcendentals=0),
        name='dw2',
    )(u, gin, part, y)


def _dw1_kernel(h_ref, z_ref, x_ref, o_ref, xo_ref):
    xo_ref[...] = x_ref[...]
    o_ref[...] = _tn(h_ref[...], z_ref[...])


def _dw1(hin, dz, dx):
    tokens, d = hin.shape
    h = dz.shape[1]
    nj = h // 1024
    rows = pl.BlockSpec((tokens // (nj * (d // 1024)), d), lambda i, j: (i * nj + j, 0))
    return pl.pallas_call(
        _dw1_kernel,
        grid=(d // 1024, nj),
        in_specs=[pl.BlockSpec((tokens, 1024), lambda i, j: (0, i)), pl.BlockSpec((tokens, 1024), lambda i, j: (0, j)), rows],
        out_specs=(pl.BlockSpec((1024, 1024), lambda i, j: (i, j)), rows),
        out_shape=(jax.ShapeDtypeStruct((d, h), F32), jax.ShapeDtypeStruct(dx.shape, BF16)),
        compiler_params=pltpu.CompilerParams(vmem_limit_bytes=VMEM_MAX, dimension_semantics=('arbitrary', 'arbitrary')),
        cost_estimate=pl.CostEstimate(flops=2 * tokens * d * h, bytes_accessed=1 << 27, transcendentals=0),
        name='dw1',
    )(hin, dz, dx)


def solution(mesh):
    def body(x, g, w1, w2):
        n_mb, mb, d = x.shape
        tokens = n_mb * mb
        b0 = tokens // CH // 2
        xt, gt = x.reshape(tokens, d), g.reshape(tokens, d)
        y, dx, hin, gin, u, dz, gp = _first_kernel(xt, gt, w1[0], w2[0], b0)
        part = _early_dw2(u, gin, tokens // 2)
        y, dx, gin, dz, part = _second_kernel(gt, w1[0], w2[0], gp, u, y, dx, gin, dz, part, b0)
        dw2, y = _dw2(u, gin, part, y, tokens // 2)
        dw1, dx = _dw1(hin, dz, dx)
        return y.reshape(x.shape), dx.reshape(x.shape), dw1[None], dw2[None]

    return jax.shard_map(body, mesh=mesh,
                         in_specs=(P('data'), P('data'), P('stage'), P('stage')),
                         out_specs=(P('data'), P('data'), P(('data', 'stage')), P(('data', 'stage'))),
                         check_vma=False)
```

```python
import functools

import jax
import jax.numpy as jnp
from jax import lax
from jax.experimental import pallas as pl
from jax.experimental.pallas import tpu as pltpu
from jax.sharding import PartitionSpec as P

MESH = pl.DeviceIdType.MESH
C0 = 0.7978845608028654
C1 = 0.044715
CH = 256
HT = 1024
DX_OP = 18
Y_FIRST = 12
Y_BLOCK = 3
DW1_EARLY = 4
EARLY = (12, 8, 4, 0)
VMEM_MAX = 67043328
F32 = jnp.float32
BF16 = jnp.bfloat16


def _nn(a, b):
    return lax.dot_general(a, b, (((1,), (0,)), ((), ())), preferred_element_type=F32)


def _nt(a, b):
    return lax.dot_general(a, b, (((1,), (1,)), ((), ())), preferred_element_type=F32)


def _tn(a, b):
    return lax.dot_general(a, b, (((0,), (0,)), ((), ())), preferred_element_type=F32)


def _gelu_parts(z):
    z2 = z * z
    p = jax.nn.sigmoid(z * (2.0 * C0 + (2.0 * C0 * C1) * z2))
    gu = z * p
    gp = p + (gu * (1.0 - p)) * (2.0 * C0 + (6.0 * C0 * C1) * z2)
    return gu.astype(BF16), gp


def _pipe_kernel(n_f, b0, n_b, *refs):
    if n_f:
        x, g, w1, w2, y, dx, hin, gin, u, dz, gp = refs[:11]
        part = part1 = None
        scratch = refs[11:]
    else:
        g, w1, w2, gp, u, hin = refs[:6]
        y, dx, gin, dz, part, part1 = refs[12:18]
        x = None
        scratch = refs[18:]
    fwd, recv_y, recv_dx, more = scratch[15:19]
    _chunks(n_f, b0, n_b, x, g, w1, w2, y, dx, hin, gin, u, dz, gp, part, part1, *scratch)
    s = lax.axis_index('stage')
    row, remote, wait_recv = _moves()
    n_ops = n_f + n_b
    dx_from = (n_ops - DX_OP + 1) // 2 if n_f else 0
    y0, n_y = (0, Y_FIRST) if n_f else (Y_FIRST, (b0 + n_b) - Y_FIRST)
    y_from = n_b if n_f else 0

    def tail_y(j, _):
        c = y0 + j

        @pl.when((s == 1) & (j >= y_from))
        def _():
            wait_recv(row(y, c), recv_y.at[j])
            remote(row(y, c), row(y, c), fwd.at[j], recv_y.at[j], 0).start()

        @pl.when((s == 0) | (s == 2))
        def _():
            wait_recv(row(y, c), recv_y.at[j])

        return 0

    def tail_dx(j, _):
        c = b0 + j

        @pl.when((s == 2) & (j >= dx_from))
        def _():
            wait_recv(row(dx, c), recv_dx.at[j])
            remote(row(dx, c), row(dx, c), fwd.at[j], recv_dx.at[j], 3).start()

        @pl.when((s == 1) | (s == 3))
        def _():
            wait_recv(row(dx, c), recv_dx.at[j])

        return 0

    lax.fori_loop(0, n_y, tail_y, 0)
    lax.fori_loop(0, n_b, tail_dx, 0)

    def drain(j, _):
        @pl.when(((s == 1) & (j < n_y)) | ((s == 2) & (j < n_b)))
        def _():
            remote(row(y, 0), row(y, 0), fwd.at[j], recv_y.at[j], 0).wait_send()

        if not n_f:
            @pl.when((s == 3) & (j < n_y))
            def _():
                remote(row(y, 0), row(y, 0), fwd.at[j], recv_y.at[j], 0).wait_send()
                remote(row(y, 0), row(y, 0), more.at[j], recv_y.at[j], 0).wait_send()

        return 0

    lax.fori_loop(0, max(n_y, n_b), drain, 0)


def _moves():
    def row(ref, c):
        return ref.at[pl.ds(pl.multiple_of(c * CH, CH), CH), :]

    def remote(src, dst, send, recv, j):
        return pltpu.make_async_remote_copy(src_ref=src, dst_ref=dst, send_sem=send, recv_sem=recv,
                                            device_id={'stage': j}, device_id_type=MESH)

    def wait_recv(dst, recv):
        remote(dst, dst, recv, recv, 0).wait_recv()

    return row, remote, wait_recv


def _per_stage(s, counts):
    return sum(jnp.where(s == i, c, 0) for i, c in enumerate(counts))


def _chunks(n_f, b0, n_b, x, g, w1, w2, y, dx, hin, gin, u, dz, gp, part, part1,
            pin_sem, w1_sem, w2_sem, in_sem, save_sem, oue, ouo, oge, ogo, ige, igo,
            snd, snd_b, loc, recv_g, fwd, recv_y, recv_dx, more,
            w1p, w2p, w1s, w2s, acc, inb, outb, gpe, gpo, ue, uo):
    recv_h = more
    row, remote, wait_recv = _moves()
    s = lax.axis_index('stage')
    first, last = s == 0, s == 3
    n_ops = n_f + n_b
    if n_f:
        warm = 16 - 8 * s + 4 * (s // 2) + 5 * (s // 3)
        pairs = jnp.minimum(n_b, n_f - warm)

    def peer(j):
        return {'stage': j}

    def op_of(k):
        if not n_f:
            return False, b0 + k
        r = k - warm
        half = r // 2
        odd = r - 2 * half
        early = k < warm
        late = r >= 2 * pairs
        late_f = warm + pairs < n_f
        is_f = early | ((odd == 1) & (~late)) | (late & late_f)
        c_late = jnp.where(late_f, warm + pairs, pairs) + r - 2 * pairs
        c = jnp.where(early, k, jnp.where(late, c_late, jnp.where(odd == 1, warm + half, half)))
        return is_f, c

    def w1_copy(t, slot):
        return pltpu.make_async_copy(w1.at[:, pl.ds(pl.multiple_of(t * HT, HT), HT)], w1s.at[slot], w1_sem.at[slot])

    def w2_copy(t, slot):
        return pltpu.make_async_copy(w2.at[pl.ds(pl.multiple_of(t * HT, HT), HT), :], w2s.at[slot], w2_sem.at[slot])

    def pin_w1(i):
        return pltpu.make_async_copy(w1.at[:, pl.ds((2 * i + 1) * HT, HT)], w1p.at[i], pin_sem.at[i])

    def pin_w2(i):
        return pltpu.make_async_copy(w2.at[pl.ds(2 * i * HT, HT), :], w2p.at[i], pin_sem.at[4 + i])

    def wait_pins(k, b):
        @pl.when(k == 0)
        def _():
            for i in range(3):
                @pl.when(b == i)
                def _():
                    pin_w2(i if n_f else i + 1).wait()
                    pin_w1(i).wait()

    def hid(ref, c, t):
        return ref.at[pl.ds(pl.multiple_of(c * CH, CH), CH), pl.ds(pl.multiple_of(t * HT, HT), HT)]

    def load_input(ref, c, slot):
        return pltpu.make_async_copy(row(ref, c), inb.at[slot], in_sem.at[slot])

    def fetch_input(k):
        is_f, c = op_of(k)
        slot = lax.rem(k, 2)
        is_b = True if not n_f else ~is_f
        if n_f:
            @pl.when(is_f & first)
            def _():
                load_input(x, c, slot).start()

            @pl.when(is_f & (s > 0))
            def _():
                wait_recv(row(hin, c), recv_h.at[c])
                load_input(hin, c, slot).start()

        @pl.when(is_b & last)
        def _():
            load_input(g, c, slot).start()

        @pl.when(is_b & (s < 3))
        def _():
            wait_recv(row(gin, c), recv_g.at[c])
            load_input(gin, c, slot).start()

        @pl.when(is_b)
        def _():
            in_gp(c, 0, *place(0)).start()

    def exits(k):
        is_f, c = op_of(k)
        if not n_f:
            return True, first, first
        share = (is_f & last & (c < Y_FIRST)) | ((~is_f) & first)
        own = (is_f & last) | ((~is_f) & first)
        return share | (~own), share, own

    def free_out(k):
        slot = lax.rem(k, 2)

        @pl.when(k >= 2)
        def _():
            one, two, own = exits(k - 2)

            @pl.when(one)
            def _():
                remote(outb.at[slot], row(gin, 0), snd.at[slot], recv_g.at[0], 0).wait_send()

            @pl.when(two)
            def _():
                remote(outb.at[slot], row(gin, 0), snd_b.at[slot], recv_g.at[0], 0).wait_send()

            @pl.when(own)
            def _():
                pltpu.make_async_copy(outb.at[slot], row(dx, 0), loc.at[slot]).wait()

    def place(t):
        return t % 2, (t - 1) // 2 % 2

    def out_u(ref, c, t, odd, slot):
        return pltpu.make_async_copy((ue, uo)[odd].at[slot], hid(ref, c, t), (oue, ouo)[odd].at[slot])

    def out_gp(c, t, odd, slot):
        return pltpu.make_async_copy((gpe, gpo)[odd].at[slot], gp.at[c, t], (oge, ogo)[odd].at[slot])

    def in_gp(c, t, odd, slot):
        return pltpu.make_async_copy(gp.at[c, t], (gpe, gpo)[odd].at[slot], (ige, igo)[odd].at[slot])

    def flush(ref, c, *tiles):
        for t in tiles:
            out_u(ref, c, t, *place(t)).wait()
            if ref is not dz:
                out_gp(c, t, *place(t)).wait()

    def emit(c, t, odd, slot):
        out_u(u, c, t, odd, slot).start()
        out_gp(c, t, odd, slot).start()

    def forward(k, c):
        slot = lax.rem(k, 2)
        load_input(x, 0, slot).wait()

        @pl.when(first)
        def _():
            pltpu.make_async_copy(inb.at[slot], row(hin, c), save_sem.at[slot]).start()

        w1_copy(0, 0).wait()
        acc[...] = inb[slot].astype(F32)
        ub, gpv = _gelu_parts(_nn(inb[slot], w1s[0]))
        ue[1] = ub
        gpe[1] = gpv
        emit(c, 0, *place(0))

        def body(b, _):
            p, q = lax.rem(b, 2), 1 - lax.rem(b, 2)
            wait_pins(k, b)
            w2_copy(2 * b + 1, p).wait()
            w1_copy(2 * b + 2, q).wait()

            @pl.when(b >= 1)
            def _():
                out_u(u, c, 2 * b - 2, 0, p).wait()
                out_gp(c, 2 * b - 2, 0, p).wait()
                w2_copy(2 * b + 3, q).start()

            @pl.when(b == 2)
            def _():
                flush(u, c, 1)

            w1_copy(lax.rem(2 * b + 4, 8), p).start()
            acc[...] += _nn(ue[q], w2p[b])
            ub, gpv = _gelu_parts(_nn(inb[slot], w1p[b]))
            uo[p] = ub
            gpo[p] = gpv
            ub, gpv = _gelu_parts(_nn(inb[slot], w1s[q]))
            ue[p] = ub
            gpe[p] = gpv
            acc[...] += _nn(uo[p], w2s[p])
            emit(c, 2 * b + 1, 1, p)
            emit(c, 2 * b + 2, 0, p)
            return 0

        lax.fori_loop(0, 3, body, 0)

        @pl.when(k == 0)
        def _():
            pin_w2(3).wait()
            pin_w1(3).wait()

        w2_copy(7, 1).wait()
        flush(u, c, 3, 4)
        free_out(k)

        @pl.when(first)
        def _():
            pltpu.make_async_copy(inb.at[slot], row(hin, c), save_sem.at[slot]).wait()

        @pl.when((k > 0) & (k + 1 < n_ops) & (k + 1 != warm))
        def _():
            fetch_input(k + 1)

        w2_copy(1, 0).start()
        w1_copy(2, 1).start()
        ub, gpv = _gelu_parts(_nn(inb[slot], w1p[3]))
        uo[1] = ub
        gpo[1] = gpv
        emit(c, 7, *place(7))
        acc[...] += _nn(ue[0], w2p[3])
        outb[slot] = (acc[...] + _nn(uo[1], w2s[1])).astype(BF16)

        @pl.when(s < 3)
        def _():
            remote(outb.at[slot], row(hin, c), snd.at[slot], recv_h.at[c], s + 1).start()

        @pl.when(last)
        def _():
            pltpu.make_async_copy(outb.at[slot], row(y, c), loc.at[slot]).start()

            @pl.when(c < Y_FIRST)
            def _():
                remote(outb.at[slot], row(y, c), snd.at[slot], recv_y.at[c], 1).start()
                remote(outb.at[slot], row(y, c), snd_b.at[slot], recv_y.at[c], 2).start()

        flush(u, c, 5, 6, 7)

        @pl.when((k == 0) | (k + 1 == warm))
        def _():
            fetch_input(k + 1)

        first_gp(k + 1)
        w2_copy(3, 1).start()

    def first_gp(k):
        is_f, c = op_of(k)

        @pl.when((k < n_ops) & (True if not n_f else ~is_f))
        def _():
            for t in (1, 2):
                in_gp(c, t, *place(t)).start()

    def pass_on_y(c):
        wait_recv(row(y, c), recv_y.at[c])
        remote(row(y, c), row(y, c), fwd.at[c], recv_y.at[c], 0).start()

    def backward(k, c):
        slot = lax.rem(k, 2)
        if n_f:
            @pl.when(s == 1)
            def _():
                pass_on_y(c)
        load_input(g, 0, slot).wait()

        @pl.when(last)
        def _():
            pltpu.make_async_copy(inb.at[slot], row(gin, c), save_sem.at[slot]).start()

        in_gp(c, 0, *place(0)).wait()
        if not n_f:
            @pl.when(k == 0)
            def _():
                pin_w2(0).wait()
        acc[...] = inb[slot].astype(F32)
        ue[1] = (_nt(inb[slot], w2p[0]) * gpe[1]).astype(BF16)
        out_u(dz, c, 0, *place(0)).start()

        def body(b, _):
            p, q = lax.rem(b, 2), 1 - lax.rem(b, 2)
            if not n_f:
                wait_pins(k, b)
            w1_copy(2 * b, p).wait()
            w2_copy(2 * b + 1, p).wait()
            in_gp(c, 2 * b + 1, 1, p).wait()
            in_gp(c, 2 * b + 2, 0, p).wait()

            @pl.when(b >= 1)
            def _():
                out_u(dz, c, 2 * b - 2, 0, p).wait()

            @pl.when(b == 2)
            def _():
                flush(dz, c, 1)

            in_gp(c, 2 * b + 3, 1, q).start()

            @pl.when(b < 2)
            def _():
                in_gp(c, 2 * b + 4, 0, q).start()

            @pl.when(b >= 1)
            def _():
                w1_copy(2 * b + 2, q).start()
                w2_copy(2 * b + 3, q).start()

            acc[...] += _nt(ue[q], w1s[p])
            uo[p] = (_nt(inb[slot], w2s[p]) * gpo[p]).astype(BF16)
            out_u(dz, c, 2 * b + 1, 1, p).start()
            ue[p] = (_nt(inb[slot], w2p[b + 1]) * gpe[p]).astype(BF16)
            out_u(dz, c, 2 * b + 2, 0, p).start()
            acc[...] += _nt(uo[p], w1p[b])
            return 0

        lax.fori_loop(0, 3, body, 0)
        if not n_f:
            @pl.when(k == 0)
            def _():
                pin_w1(3).wait()
        w1_copy(6, 1).wait()
        w2_copy(7, 1).wait()
        in_gp(c, 7, *place(7)).wait()
        flush(dz, c, 3, 4)
        free_out(k)

        @pl.when(last)
        def _():
            pltpu.make_async_copy(inb.at[slot], row(gin, c), save_sem.at[slot]).wait()

        @pl.when(k + 1 < n_ops)
        def _():
            fetch_input(k + 1)

        w1_copy(0, 0).start()
        w2_copy(1, 0).start()
        uo[1] = (_nt(inb[slot], w2s[1]) * gpo[1]).astype(BF16)
        out_u(dz, c, 7, *place(7)).start()
        acc[...] += _nt(ue[0], w1s[1])
        outb[slot] = (acc[...] + _nt(uo[1], w1p[3])).astype(BF16)
        if not n_f:
            @pl.when(k == 0)
            def _():
                pl.semaphore_wait(barrier, 2 - (s == 1).astype(jnp.int32))

        @pl.when(s > 0)
        def _():
            remote(outb.at[slot], row(gin, c), snd.at[slot], recv_g.at[c], s - 1).start()

        @pl.when(first)
        def _():
            pltpu.make_async_copy(outb.at[slot], row(dx, c), loc.at[slot]).start()
            remote(outb.at[slot], row(dx, c), snd.at[slot], recv_dx.at[c - b0], 2).start()
            remote(outb.at[slot], row(dx, c), snd_b.at[slot], recv_dx.at[c - b0], 1).start()

        first_gp(k + 1)
        w1_copy(2, 1).start()
        w2_copy(3, 1).start()
        flush(dz, c, 5, 6, 7)

    def half_blocks(lo):
        half, n2 = w1p.shape[1], u.shape[1] // HT
        hi = n2 + DW1_EARLY

        def cols(ref, i, n):
            return ref.at[pl.ds(0, half), pl.ds(pl.multiple_of(i * HT, HT), n * HT)]

        def loads(i, a, b):
            slot = lax.rem(i - lo, 2)
            return [pltpu.make_async_copy(a, w1s.at[slot], w1_sem.at[slot])] + [
                pltpu.make_async_copy(b.at[:, pl.ds(j * HT, HT)], w1p.at[2 * slot + j], pin_sem.at[2 * slot + j]) for j in range(2)]

        def start(i):
            @pl.when(i < n2)
            def _():
                for copy in loads(i, cols(u, i, 1), cols(gin, 0, 2)):
                    copy.start()

            @pl.when(i >= n2)
            def _():
                j = (i - n2) // 2
                for copy in loads(i, cols(hin, i - n2 - 2 * j, 1), cols(dz, 2 * j, 2)):
                    copy.start()

        def outs(i, row, p, dst, col):
            rows = pl.ds(pl.multiple_of(row, CH), CH)
            return [pltpu.make_async_copy(buf.at[p], dst.at[rows, pl.ds(pl.multiple_of(col + j * HT, HT), HT)], sem.at[p])
                    for j, (buf, sem) in enumerate(((gpe, oge), (gpo, ogo)))]

        def finish(p):
            for copy in outs(lo, 0, p, part, 0):
                copy.wait()

        @pl.when(lo < hi)
        def _():
            start(lo)

            def block(i, _):
                slot = lax.rem(i - lo, 2)

                @pl.when(i + 1 < hi)
                def _():
                    start(i + 1)

                for copy in loads(i, cols(u, 0, 1), cols(gin, 0, 2)):
                    copy.wait()

                @pl.when(last & (i == lo + Y_BLOCK))
                def _():
                    for j in range(b0 + n_b - Y_FIRST):
                        yj = row(y, Y_FIRST + j)
                        remote(yj, yj, fwd.at[j], recv_y.at[j], 1).start()
                        remote(yj, yj, more.at[j], recv_y.at[j], 2).start()

                def strip(j, _):
                    p = lax.rem(j, 2)

                    @pl.when((i > lo) | (j > 1))
                    def _():
                        finish(p)

                    lhs = w1s[slot, :, pl.ds(pl.multiple_of(j * CH, CH), CH)]
                    gpe[p] = _tn(lhs, w1p[2 * slot])
                    gpo[p] = _tn(lhs, w1p[2 * slot + 1])
                    r = i - n2
                    j1 = r // 2

                    @pl.when(r < 0)
                    def _():
                        for copy in outs(i, i * HT + j * CH, p, part, 0):
                            copy.start()

                    @pl.when(r >= 0)
                    def _():
                        for copy in outs(i, (r - 2 * j1) * HT + j * CH, p, part1, 2 * j1 * HT):
                            copy.start()

                    return 0

                lax.fori_loop(0, HT // CH, strip, 0)
                return 0

            lax.fori_loop(lo, hi, block, 0)
            finish(0)
            finish(1)

    barrier = pltpu.get_barrier_semaphore()
    if n_f:
        @pl.when(first)
        def _():
            fetch_input(0)
        w1_copy(0, 0).start()
        for i in range(4):
            pin_w2(i).start()
            pin_w1(i).start()
            if i == 0:
                w2_copy(1, 0).start()
                w1_copy(2, 1).start()
            if i == 1:
                w2_copy(3, 1).start()
        for d in range(1, 4):
            pl.semaphore_signal(barrier, inc=1, device_id=peer(lax.rem(s + d, 4)), device_id_type=MESH)
        pl.semaphore_wait(barrier, 3)

        @pl.when(s > 0)
        def _():
            fetch_input(0)
    else:
        for to, frm in ((1, 0), (2, 1), (3, 1), (0, 1), (3, 2), (0, 2), (2, 3)):
            @pl.when(s == frm)
            def _():
                pl.semaphore_signal(barrier, inc=1, device_id=peer(to), device_id_type=MESH)
        @pl.when(last)
        def _():
            fetch_input(0)
        pin_w2(0).start()
        w1_copy(0, 0).start()
        w2_copy(1, 0).start()
        pin_w1(0).start()
        pin_w2(1).start()
        first_gp(0)
        w1_copy(2, 1).start()
        w2_copy(3, 1).start()
        for i in range(1, 4):
            pin_w1(i).start()
            if i < 3:
                pin_w2(i + 1).start()

        @pl.when(s < 3)
        def _():
            fetch_input(0)

    def step(k, _):
        is_f, c = op_of(k)
        if not n_f:
            backward(k, c)
            return 0
        gone = k - DX_OP
        cd = gone // 2

        @pl.when((s == 2) & (gone >= 0) & (gone == 2 * cd) & (gone < 2 * n_b))
        def _():
            wait_recv(row(dx, cd), recv_dx.at[cd])
            remote(row(dx, cd), row(dx, cd), fwd.at[cd], recv_dx.at[cd], 3).start()

        @pl.when(is_f)
        def _():
            forward(k, c)

        @pl.when(~is_f)
        def _():
            backward(k, c)

        return 0

    lax.fori_loop(0, n_ops, step, 0)

    w1_copy(0, 0).wait()
    w1_copy(2, 1).wait()
    w2_copy(1, 0).wait()
    w2_copy(3, 1).wait()
    free_out(n_ops)
    free_out(n_ops + 1)
    if not n_f:
        half_blocks(_per_stage(s, EARLY))


def _scratch(nc, n_b, d, n_f):
    dma = pltpu.SemaphoreType.DMA
    sems = [dma((8,)), *[dma((2,))] * 13, *[dma((nc,))] * 5]
    return sems + [
        pltpu.VMEM((4, d, HT), BF16), pltpu.VMEM((4, HT, d), BF16),
        pltpu.VMEM((2, d, HT), BF16), pltpu.VMEM((2, HT, d), BF16),
        pltpu.VMEM((CH, d), F32), pltpu.VMEM((2, CH, d), BF16), pltpu.VMEM((2, CH, d), BF16),
        pltpu.VMEM((2, CH, HT), F32), pltpu.VMEM((2, CH, HT), F32),
        pltpu.VMEM((2, CH, HT), BF16), pltpu.VMEM((2, CH, HT), BF16)]


def _first_kernel(x, g, w1, w2, n_b):
    tokens, d = x.shape
    h = w1.shape[1]
    nc = tokens // CH
    rows = jax.ShapeDtypeStruct((tokens, d), BF16)
    wide = jax.ShapeDtypeStruct((tokens, h), BF16)
    anyspec = pl.BlockSpec(memory_space=pl.ANY)
    return pl.pallas_call(
        functools.partial(_pipe_kernel, nc, 0, n_b),
        out_shape=(rows, rows, rows, rows, wide, wide, jax.ShapeDtypeStruct((nc, h // HT, CH, HT), F32)),
        in_specs=[anyspec] * 4,
        out_specs=(anyspec,) * 7,
        scratch_shapes=_scratch(nc, n_b, d, nc),
        compiler_params=pltpu.CompilerParams(collective_id=0, has_side_effects=True, vmem_limit_bytes=VMEM_MAX),
        name='pipe_a',
    )(x, g, w1, w2)


def _second_kernel(g, w1, w2, gp, u, hin, y, dx, gin, dz, part, part1, b0):
    tokens, d = g.shape
    nc = tokens // CH
    n_b = nc - b0
    anyspec = pl.BlockSpec(memory_space=pl.ANY)
    both = (y, dx, gin, dz, part, part1)
    return pl.pallas_call(
        functools.partial(_pipe_kernel, 0, b0, n_b),
        out_shape=tuple(jax.ShapeDtypeStruct(a.shape, a.dtype) for a in both),
        in_specs=[anyspec] * 12,
        out_specs=(anyspec,) * len(both),
        scratch_shapes=_scratch(nc, n_b, d, 0),
        input_output_aliases={6 + i: i for i in range(len(both))},
        compiler_params=pltpu.CompilerParams(collective_id=1, has_side_effects=True, vmem_limit_bytes=VMEM_MAX),
        name='pipe_b',
    )(g, w1, w2, gp, u, hin, *both)


def _product(a_ref, b_ref, o_ref):
    o_ref[...] = _tn(a_ref[...], b_ref[...])


def _early_kernel(half, u, g, hin, dz, o, o1):
    n = _per_stage(lax.axis_index('stage'), EARLY)
    d = g.shape[1]
    n2, nd = u.shape[1] // HT, d // HT

    @pl.when(n > 0)
    def _():
        pltpu.emit_pipeline(
            _product, grid=(jnp.minimum(n, n2),),
            in_specs=[pl.BlockSpec((half, HT), lambda i: (0, i)), pl.BlockSpec((half, d), lambda i: (0, 0))],
            out_specs=[pl.BlockSpec((HT, d), lambda i: (i, 0))])(u, g, o)

    @pl.when(n > n2)
    def _():
        pltpu.emit_pipeline(
            _product, grid=(n - n2,),
            in_specs=[pl.BlockSpec((half, HT), lambda i: (0, lax.rem(i, nd))), pl.BlockSpec((half, d), lambda i: (0, lax.div(i, nd)))],
            out_specs=[pl.BlockSpec((HT, d), lambda i: (lax.rem(i, nd), lax.div(i, nd)))])(hin, dz, o1)


def _early(u, gin, hin, dz, half):
    h, d = u.shape[1], gin.shape[1]
    anyspec = pl.BlockSpec(memory_space=pl.ANY)
    return pl.pallas_call(
        functools.partial(_early_kernel, half),
        in_specs=[anyspec] * 4,
        out_specs=(anyspec,) * 2,
        out_shape=(jax.ShapeDtypeStruct((h, d), F32), jax.ShapeDtypeStruct((d, h), F32)),
        compiler_params=pltpu.CompilerParams(vmem_limit_bytes=VMEM_MAX),
        name='early',
    )(u, gin, hin, dz)


def _dw2_kernel(u_ref, g_ref, part_ref, y_ref, o_ref, yo_ref):
    yo_ref[...] = y_ref[...]
    o_ref[...] = part_ref[...] + _tn(u_ref[...], g_ref[...])


def _dw2(u, gin, part, y, half):
    tokens, h = u.shape
    d = gin.shape[1]
    steps = h // HT
    rows = pl.BlockSpec((tokens // steps, d), lambda i: (i, 0))
    blocks = pl.BlockSpec((HT, d), lambda i: (i, 0))
    return pl.pallas_call(
        _dw2_kernel,
        grid=(steps,),
        in_specs=[pl.BlockSpec((half, HT), lambda i: (1, i)),
                  pl.BlockSpec((half, d), lambda i: (1, 0), pipeline_mode=pl.Buffered(1)), blocks, rows],
        out_specs=(blocks, rows),
        out_shape=(jax.ShapeDtypeStruct((h, d), F32), jax.ShapeDtypeStruct(y.shape, BF16)),
        compiler_params=pltpu.CompilerParams(vmem_limit_bytes=VMEM_MAX, dimension_semantics=('arbitrary',)),
        name='dw2',
    )(u, gin, part, y)


def _dw1_late_kernel(h_ref, z_ref, part_ref, o_ref):
    o_ref[...] = part_ref[...] + _tn(h_ref[...], z_ref[...])


def _dw1_kernel(h_ref, z_ref, x_ref, _, o_ref, xo_ref):
    xo_ref[...] = x_ref[...]
    o_ref[...] = _tn(h_ref[...], z_ref[...])


def _dw1(hin, dz, part1, dx, half):
    tokens, d = hin.shape
    h = dz.shape[1]
    nd = d // HT
    blocks = pl.BlockSpec((HT, d), lambda i: (lax.rem(i, nd), lax.div(i, nd)))
    out = jax.ShapeDtypeStruct((d, h), F32)
    done = pl.pallas_call(
        _dw1_late_kernel,
        grid=(DW1_EARLY,),
        in_specs=[pl.BlockSpec((half, HT), lambda i: (1, lax.rem(i, nd))), pl.BlockSpec((half, d), lambda i: (1, lax.div(i, nd))), blocks],
        out_specs=blocks,
        out_shape=out,
        compiler_params=pltpu.CompilerParams(vmem_limit_bytes=VMEM_MAX, dimension_semantics=('arbitrary',)),
        name='dw1_late',
    )(hin, dz, part1)
    nj = h // HT - DW1_EARLY
    j0 = DW1_EARLY
    rows = pl.BlockSpec((tokens // (nj * nd), d), lambda i, j: (i * nj + j, 0))
    return pl.pallas_call(
        _dw1_kernel,
        grid=(nd, nj),
        in_specs=[pl.BlockSpec((tokens, HT), lambda i, j: (0, i)), pl.BlockSpec((tokens, HT), lambda i, j: (0, j0 + j)), rows,
                  pl.BlockSpec(memory_space=pl.ANY)],
        out_specs=(pl.BlockSpec((HT, HT), lambda i, j: (i, j0 + j)), rows),
        out_shape=(out, jax.ShapeDtypeStruct(dx.shape, BF16)),
        input_output_aliases={3: 0},
        compiler_params=pltpu.CompilerParams(vmem_limit_bytes=VMEM_MAX, dimension_semantics=('arbitrary', 'arbitrary')),
        name='dw1',
    )(hin, dz, dx, done)


def solution(mesh):
    def body(x, g, w1, w2):
        n_mb, mb, d = x.shape
        tokens = n_mb * mb
        b0 = tokens // CH // 2
        xt, gt = x.reshape(tokens, d), g.reshape(tokens, d)
        y, dx, hin, gin, u, dz, gp = _first_kernel(xt, gt, w1[0], w2[0], b0)
        half = tokens // 2
        part, part1 = _early(u, gin, hin, dz, half)
        y, dx, gin, dz, part, part1 = _second_kernel(gt, w1[0], w2[0], gp, u, hin, y, dx, gin, dz, part, part1, b0)
        dw2, y = _dw2(u, gin, part, y, half)
        dw1, dx = _dw1(hin, dz, part1, dx, half)
        return y.reshape(x.shape), dx.reshape(x.shape), dw1[None], dw2[None]

    return jax.shard_map(body, mesh=mesh,
                         in_specs=(P('data'), P('data'), P('stage'), P('stage')),
                         out_specs=(P('data'), P('data'), P(('data', 'stage')), P(('data', 'stage'))),
                         check_vma=False)
```

```python
import functools

import jax
import jax.numpy as jnp
from jax import lax
from jax.experimental import pallas as pl
from jax.experimental.pallas import tpu as pltpu
from jax.sharding import PartitionSpec as P

MESH = pl.DeviceIdType.MESH
C0 = 0.7978845608028654
C1 = 0.044715
CH = 256
HT = 1024
DX_OP = 18
Y_FIRST = 12
Y_BLOCK = 3
DW1_EARLY = 4
EARLY = (11, 8, 4, 0)
VMEM_MAX = 67043328
F32 = jnp.float32
BF16 = jnp.bfloat16


def _nn(a, b):
    return lax.dot_general(a, b, (((1,), (0,)), ((), ())), preferred_element_type=F32)


def _nt(a, b):
    return lax.dot_general(a, b, (((1,), (1,)), ((), ())), preferred_element_type=F32)


def _tn(a, b):
    return lax.dot_general(a, b, (((0,), (0,)), ((), ())), preferred_element_type=F32)


def _gelu_parts(z):
    z2 = z * z
    p = jax.nn.sigmoid(z * (2.0 * C0 + (2.0 * C0 * C1) * z2))
    gu = z * p
    gp = p + (gu * (1.0 - p)) * (2.0 * C0 + (6.0 * C0 * C1) * z2)
    return gu.astype(BF16), gp


def _pipe_kernel(n_f, b0, n_b, *refs):
    if n_f:
        x, g, w1, w2, y, dx, hin, gin, u, dz, gp = refs[:11]
        part = part1 = None
        scratch = refs[11:]
    else:
        g, w1, w2, gp, u, hin = refs[:6]
        y, dx, gin, dz, part, part1 = refs[12:18]
        x = None
        scratch = refs[18:]
    fwd, recv_y, recv_dx, more = scratch[15:19]
    _chunks(n_f, b0, n_b, x, g, w1, w2, y, dx, hin, gin, u, dz, gp, part, part1, *scratch)
    s = lax.axis_index('stage')
    row, remote, wait_recv = _moves()
    n_ops = n_f + n_b
    dx_from = (n_ops - DX_OP + 1) // 2 if n_f else 0
    y0, n_y = (0, Y_FIRST) if n_f else (Y_FIRST, (b0 + n_b) - Y_FIRST)
    y_from = n_b if n_f else 0

    def tail_y(j, _):
        c = y0 + j

        @pl.when((s == 1) & (j >= y_from))
        def _():
            wait_recv(row(y, c), recv_y.at[j])
            remote(row(y, c), row(y, c), fwd.at[j], recv_y.at[j], 0).start()

        @pl.when((s == 0) | (s == 2))
        def _():
            wait_recv(row(y, c), recv_y.at[j])

        return 0

    def tail_dx(j, _):
        c = b0 + j

        @pl.when((s == 2) & (j >= dx_from))
        def _():
            wait_recv(row(dx, c), recv_dx.at[j])
            remote(row(dx, c), row(dx, c), fwd.at[j], recv_dx.at[j], 3).start()

        @pl.when((s == 1) | (s == 3))
        def _():
            wait_recv(row(dx, c), recv_dx.at[j])

        return 0

    lax.fori_loop(0, n_y, tail_y, 0)
    lax.fori_loop(0, n_b, tail_dx, 0)

    def drain(j, _):
        @pl.when(((s == 1) & (j < n_y)) | ((s == 2) & (j < n_b)))
        def _():
            remote(row(y, 0), row(y, 0), fwd.at[j], recv_y.at[j], 0).wait_send()

        if not n_f:
            @pl.when((s == 3) & (j < n_y))
            def _():
                remote(row(y, 0), row(y, 0), fwd.at[j], recv_y.at[j], 0).wait_send()
                remote(row(y, 0), row(y, 0), more.at[j], recv_y.at[j], 0).wait_send()

        return 0

    lax.fori_loop(0, max(n_y, n_b), drain, 0)


def _moves():
    def row(ref, c):
        return ref.at[pl.ds(pl.multiple_of(c * CH, CH), CH), :]

    def remote(src, dst, send, recv, j):
        return pltpu.make_async_remote_copy(src_ref=src, dst_ref=dst, send_sem=send, recv_sem=recv,
                                            device_id={'stage': j}, device_id_type=MESH)

    def wait_recv(dst, recv):
        remote(dst, dst, recv, recv, 0).wait_recv()

    return row, remote, wait_recv


def _per_stage(s, counts):
    return sum(jnp.where(s == i, c, 0) for i, c in enumerate(counts))


def _chunks(n_f, b0, n_b, x, g, w1, w2, y, dx, hin, gin, u, dz, gp, part, part1,
            pin_sem, w1_sem, w2_sem, in_sem, save_sem, oue, ouo, oge, ogo, ige, igo,
            snd, snd_b, loc, recv_g, fwd, recv_y, recv_dx, more,
            w1p, w2p, w1s, w2s, acc, inb, outb, gpe, gpo, ue, uo):
    recv_h = more
    row, remote, wait_recv = _moves()
    s = lax.axis_index('stage')
    first, last = s == 0, s == 3
    n_ops = n_f + n_b
    if n_f:
        warm = 16 - 4 * s - 4 * (s // 2) + (s // 3)
        pairs = jnp.minimum(n_b, n_f - warm)

    def peer(j):
        return {'stage': j}

    def op_of(k):
        if not n_f:
            return False, b0 + k
        r = k - warm
        half = r // 2
        odd = r - 2 * half
        early = k < warm
        late = r >= 2 * pairs
        late_f = warm + pairs < n_f
        is_f = early | ((odd == 1) & (~late)) | (late & late_f)
        c_late = jnp.where(late_f, warm + pairs, pairs) + r - 2 * pairs
        c = jnp.where(early, k, jnp.where(late, c_late, jnp.where(odd == 1, warm + half, half)))
        return is_f, c

    def w1_copy(t, slot):
        return pltpu.make_async_copy(w1.at[:, pl.ds(pl.multiple_of(t * HT, HT), HT)], w1s.at[slot], w1_sem.at[slot])

    def w2_copy(t, slot):
        return pltpu.make_async_copy(w2.at[pl.ds(pl.multiple_of(t * HT, HT), HT), :], w2s.at[slot], w2_sem.at[slot])

    def pin_w1(i):
        return pltpu.make_async_copy(w1.at[:, pl.ds((2 * i + 1) * HT, HT)], w1p.at[i], pin_sem.at[i])

    def pin_w2(i):
        return pltpu.make_async_copy(w2.at[pl.ds(2 * i * HT, HT), :], w2p.at[i], pin_sem.at[4 + i])

    def wait_pins(k, b):
        @pl.when(k == 0)
        def _():
            for i in range(3):
                @pl.when(b == i)
                def _():
                    pin_w2(i if n_f else i + 1).wait()
                    pin_w1(i).wait()

    def hid(ref, c, t):
        return ref.at[pl.ds(pl.multiple_of(c * CH, CH), CH), pl.ds(pl.multiple_of(t * HT, HT), HT)]

    def load_input(ref, c, slot):
        return pltpu.make_async_copy(row(ref, c), inb.at[slot], in_sem.at[slot])

    def fetch_input(k):
        is_f, c = op_of(k)
        slot = lax.rem(k, 2)
        is_b = True if not n_f else ~is_f
        if n_f:
            @pl.when(is_f & first)
            def _():
                load_input(x, c, slot).start()

            @pl.when(is_f & (s > 0))
            def _():
                wait_recv(row(hin, c), recv_h.at[c])
                load_input(hin, c, slot).start()

        @pl.when(is_b & last)
        def _():
            load_input(g, c, slot).start()

        @pl.when(is_b & (s < 3))
        def _():
            wait_recv(row(gin, c), recv_g.at[c])
            load_input(gin, c, slot).start()

        @pl.when(is_b)
        def _():
            in_gp(c, 0, *place(0)).start()

    def exits(k):
        is_f, c = op_of(k)
        if not n_f:
            return True, first, first
        share = (is_f & last & (c < Y_FIRST)) | ((~is_f) & first)
        own = (is_f & last) | ((~is_f) & first)
        return share | (~own), share, own

    def free_out(k):
        slot = lax.rem(k, 2)

        @pl.when(k >= 2)
        def _():
            one, two, own = exits(k - 2)

            @pl.when(one)
            def _():
                remote(outb.at[slot], row(gin, 0), snd.at[slot], recv_g.at[0], 0).wait_send()

            @pl.when(two)
            def _():
                remote(outb.at[slot], row(gin, 0), snd_b.at[slot], recv_g.at[0], 0).wait_send()

            @pl.when(own)
            def _():
                pltpu.make_async_copy(outb.at[slot], row(dx, 0), loc.at[slot]).wait()

    def place(t):
        return t % 2, (t - 1) // 2 % 2

    def out_u(ref, c, t, odd, slot):
        return pltpu.make_async_copy((ue, uo)[odd].at[slot], hid(ref, c, t), (oue, ouo)[odd].at[slot])

    def out_gp(c, t, odd, slot):
        return pltpu.make_async_copy((gpe, gpo)[odd].at[slot], gp.at[c, t], (oge, ogo)[odd].at[slot])

    def in_gp(c, t, odd, slot):
        return pltpu.make_async_copy(gp.at[c, t], (gpe, gpo)[odd].at[slot], (ige, igo)[odd].at[slot])

    def flush(ref, c, *tiles):
        for t in tiles:
            out_u(ref, c, t, *place(t)).wait()
            if ref is not dz:
                out_gp(c, t, *place(t)).wait()

    def emit(c, t, odd, slot):
        out_u(u, c, t, odd, slot).start()
        out_gp(c, t, odd, slot).start()

    def forward(k, c):
        slot = lax.rem(k, 2)
        load_input(x, 0, slot).wait()

        @pl.when(first)
        def _():
            pltpu.make_async_copy(inb.at[slot], row(hin, c), save_sem.at[slot]).start()

        w1_copy(0, 0).wait()
        acc[...] = inb[slot].astype(F32)
        ub, gpv = _gelu_parts(_nn(inb[slot], w1s[0]))
        ue[1] = ub
        gpe[1] = gpv
        emit(c, 0, *place(0))

        def body(b, _):
            p, q = lax.rem(b, 2), 1 - lax.rem(b, 2)
            wait_pins(k, b)
            w2_copy(2 * b + 1, p).wait()
            w1_copy(2 * b + 2, q).wait()

            @pl.when(b >= 1)
            def _():
                out_u(u, c, 2 * b - 2, 0, p).wait()
                out_gp(c, 2 * b - 2, 0, p).wait()
                w2_copy(2 * b + 3, q).start()

            @pl.when(b == 2)
            def _():
                flush(u, c, 1)

            w1_copy(lax.rem(2 * b + 4, 8), p).start()
            acc[...] += _nn(ue[q], w2p[b])
            ub, gpv = _gelu_parts(_nn(inb[slot], w1p[b]))
            uo[p] = ub
            gpo[p] = gpv
            ub, gpv = _gelu_parts(_nn(inb[slot], w1s[q]))
            ue[p] = ub
            gpe[p] = gpv
            acc[...] += _nn(uo[p], w2s[p])
            emit(c, 2 * b + 1, 1, p)
            emit(c, 2 * b + 2, 0, p)
            return 0

        lax.fori_loop(0, 3, body, 0)

        @pl.when(k == 0)
        def _():
            pin_w2(3).wait()
            pin_w1(3).wait()

        w2_copy(7, 1).wait()
        flush(u, c, 3, 4)
        free_out(k)

        @pl.when(first)
        def _():
            pltpu.make_async_copy(inb.at[slot], row(hin, c), save_sem.at[slot]).wait()

        @pl.when((k > 0) & (k + 1 < n_ops) & (k + 1 != warm))
        def _():
            fetch_input(k + 1)

        w2_copy(1, 0).start()
        w1_copy(2, 1).start()
        ub, gpv = _gelu_parts(_nn(inb[slot], w1p[3]))
        uo[1] = ub
        gpo[1] = gpv
        emit(c, 7, *place(7))
        acc[...] += _nn(ue[0], w2p[3])
        outb[slot] = (acc[...] + _nn(uo[1], w2s[1])).astype(BF16)

        @pl.when(s < 3)
        def _():
            remote(outb.at[slot], row(hin, c), snd.at[slot], recv_h.at[c], s + 1).start()

        @pl.when(last)
        def _():
            pltpu.make_async_copy(outb.at[slot], row(y, c), loc.at[slot]).start()

            @pl.when(c < Y_FIRST)
            def _():
                remote(outb.at[slot], row(y, c), snd.at[slot], recv_y.at[c], 1).start()
                remote(outb.at[slot], row(y, c), snd_b.at[slot], recv_y.at[c], 2).start()

        flush(u, c, 5, 6, 7)

        @pl.when((k == 0) | (k + 1 == warm))
        def _():
            fetch_input(k + 1)

        first_gp(k + 1)
        w2_copy(3, 1).start()

    def first_gp(k):
        is_f, c = op_of(k)

        @pl.when((k < n_ops) & (True if not n_f else ~is_f))
        def _():
            for t in (1, 2):
                in_gp(c, t, *place(t)).start()

    def pass_on_y(c):
        wait_recv(row(y, c), recv_y.at[c])
        remote(row(y, c), row(y, c), fwd.at[c], recv_y.at[c], 0).start()

    def backward(k, c):
        slot = lax.rem(k, 2)
        if n_f:
            @pl.when(s == 1)
            def _():
                pass_on_y(c)
        load_input(g, 0, slot).wait()

        @pl.when(last)
        def _():
            pltpu.make_async_copy(inb.at[slot], row(gin, c), save_sem.at[slot]).start()

        in_gp(c, 0, *place(0)).wait()
        if not n_f:
            @pl.when(k == 0)
            def _():
                pin_w2(0).wait()
        acc[...] = inb[slot].astype(F32)
        ue[1] = (_nt(inb[slot], w2p[0]) * gpe[1]).astype(BF16)
        out_u(dz, c, 0, *place(0)).start()

        def body(b, _):
            p, q = lax.rem(b, 2), 1 - lax.rem(b, 2)
            if not n_f:
                wait_pins(k, b)
            w1_copy(2 * b, p).wait()
            w2_copy(2 * b + 1, p).wait()
            in_gp(c, 2 * b + 1, 1, p).wait()
            in_gp(c, 2 * b + 2, 0, p).wait()

            @pl.when(b >= 1)
            def _():
                out_u(dz, c, 2 * b - 2, 0, p).wait()

            @pl.when(b == 2)
            def _():
                flush(dz, c, 1)

            in_gp(c, 2 * b + 3, 1, q).start()

            @pl.when(b < 2)
            def _():
                in_gp(c, 2 * b + 4, 0, q).start()

            @pl.when(b >= 1)
            def _():
                w1_copy(2 * b + 2, q).start()
                w2_copy(2 * b + 3, q).start()

            acc[...] += _nt(ue[q], w1s[p])
            uo[p] = (_nt(inb[slot], w2s[p]) * gpo[p]).astype(BF16)
            out_u(dz, c, 2 * b + 1, 1, p).start()
            ue[p] = (_nt(inb[slot], w2p[b + 1]) * gpe[p]).astype(BF16)
            out_u(dz, c, 2 * b + 2, 0, p).start()
            acc[...] += _nt(uo[p], w1p[b])
            return 0

        lax.fori_loop(0, 3, body, 0)
        if not n_f:
            @pl.when(k == 0)
            def _():
                pin_w1(3).wait()
        w1_copy(6, 1).wait()
        w2_copy(7, 1).wait()
        in_gp(c, 7, *place(7)).wait()
        flush(dz, c, 3, 4)
        free_out(k)

        @pl.when(last)
        def _():
            pltpu.make_async_copy(inb.at[slot], row(gin, c), save_sem.at[slot]).wait()

        @pl.when(k + 1 < n_ops)
        def _():
            fetch_input(k + 1)

        w1_copy(0, 0).start()
        w2_copy(1, 0).start()
        uo[1] = (_nt(inb[slot], w2s[1]) * gpo[1]).astype(BF16)
        out_u(dz, c, 7, *place(7)).start()
        acc[...] += _nt(ue[0], w1s[1])
        outb[slot] = (acc[...] + _nt(uo[1], w1p[3])).astype(BF16)
        if not n_f:
            @pl.when(k == 0)
            def _():
                pl.semaphore_wait(barrier, 2 - (s == 1).astype(jnp.int32))

        @pl.when(s > 0)
        def _():
            remote(outb.at[slot], row(gin, c), snd.at[slot], recv_g.at[c], s - 1).start()

        @pl.when(first)
        def _():
            pltpu.make_async_copy(outb.at[slot], row(dx, c), loc.at[slot]).start()
            remote(outb.at[slot], row(dx, c), snd.at[slot], recv_dx.at[c - b0], 2).start()
            remote(outb.at[slot], row(dx, c), snd_b.at[slot], recv_dx.at[c - b0], 1).start()

        first_gp(k + 1)
        w1_copy(2, 1).start()
        w2_copy(3, 1).start()
        flush(dz, c, 5, 6, 7)

    def half_blocks(lo):
        half, n2 = w1p.shape[1], u.shape[1] // HT
        hi = n2 + DW1_EARLY

        def cols(ref, i, n):
            return ref.at[pl.ds(0, half), pl.ds(pl.multiple_of(i * HT, HT), n * HT)]

        def loads(i, a, b):
            slot = lax.rem(i - lo, 2)
            return [pltpu.make_async_copy(a, w1s.at[slot], w1_sem.at[slot])] + [
                pltpu.make_async_copy(b.at[:, pl.ds(j * HT, HT)], w1p.at[2 * slot + j], pin_sem.at[2 * slot + j]) for j in range(2)]

        def start(i):
            @pl.when(i < n2)
            def _():
                for copy in loads(i, cols(u, i, 1), cols(gin, 0, 2)):
                    copy.start()

            @pl.when(i >= n2)
            def _():
                j = (i - n2) // 2
                for copy in loads(i, cols(hin, i - n2 - 2 * j, 1), cols(dz, 2 * j, 2)):
                    copy.start()

        def outs(i, row, p, dst, col):
            rows = pl.ds(pl.multiple_of(row, CH), CH)
            return [pltpu.make_async_copy(buf.at[p], dst.at[rows, pl.ds(pl.multiple_of(col + j * HT, HT), HT)], sem.at[p])
                    for j, (buf, sem) in enumerate(((gpe, oge), (gpo, ogo)))]

        def finish(p):
            for copy in outs(lo, 0, p, part, 0):
                copy.wait()

        @pl.when(lo < hi)
        def _():
            start(lo)

            def block(i, _):
                slot = lax.rem(i - lo, 2)

                @pl.when(i + 1 < hi)
                def _():
                    start(i + 1)

                for copy in loads(i, cols(u, 0, 1), cols(gin, 0, 2)):
                    copy.wait()

                @pl.when(last & (i == lo + Y_BLOCK))
                def _():
                    for j in range(b0 + n_b - Y_FIRST):
                        yj = row(y, Y_FIRST + j)
                        remote(yj, yj, fwd.at[j], recv_y.at[j], 1).start()
                        remote(yj, yj, more.at[j], recv_y.at[j], 2).start()

                def strip(j, _):
                    p = lax.rem(j, 2)

                    @pl.when((i > lo) | (j > 1))
                    def _():
                        finish(p)

                    lhs = w1s[slot, :, pl.ds(pl.multiple_of(j * CH, CH), CH)]
                    gpe[p] = _tn(lhs, w1p[2 * slot])
                    gpo[p] = _tn(lhs, w1p[2 * slot + 1])
                    r = i - n2
                    j1 = r // 2

                    @pl.when(r < 0)
                    def _():
                        for copy in outs(i, i * HT + j * CH, p, part, 0):
                            copy.start()

                    @pl.when(r >= 0)
                    def _():
                        for copy in outs(i, (r - 2 * j1) * HT + j * CH, p, part1, 2 * j1 * HT):
                            copy.start()

                    return 0

                lax.fori_loop(0, HT // CH, strip, 0)
                return 0

            lax.fori_loop(lo, hi, block, 0)
            finish(0)
            finish(1)

    barrier = pltpu.get_barrier_semaphore()
    if n_f:
        @pl.when(first)
        def _():
            fetch_input(0)
        w1_copy(0, 0).start()
        for i in range(4):
            pin_w2(i).start()
            pin_w1(i).start()
            if i == 0:
                w2_copy(1, 0).start()
                w1_copy(2, 1).start()
            if i == 1:
                w2_copy(3, 1).start()
        for d in range(1, 4):
            pl.semaphore_signal(barrier, inc=1, device_id=peer(lax.rem(s + d, 4)), device_id_type=MESH)
        pl.semaphore_wait(barrier, 3)

        @pl.when(s > 0)
        def _():
            fetch_input(0)
    else:
        for to, frm in ((1, 0), (2, 1), (3, 1), (0, 1), (3, 2), (0, 2), (2, 3)):
            @pl.when(s == frm)
            def _():
                pl.semaphore_signal(barrier, inc=1, device_id=peer(to), device_id_type=MESH)
        @pl.when(last)
        def _():
            fetch_input(0)
        pin_w2(0).start()
        w1_copy(0, 0).start()
        w2_copy(1, 0).start()
        pin_w1(0).start()
        pin_w2(1).start()
        first_gp(0)
        w1_copy(2, 1).start()
        w2_copy(3, 1).start()
        for i in range(1, 4):
            pin_w1(i).start()
            if i < 3:
                pin_w2(i + 1).start()

        @pl.when(s < 3)
        def _():
            fetch_input(0)

    def step(k, _):
        is_f, c = op_of(k)
        if not n_f:
            backward(k, c)
            return 0
        gone = k - DX_OP
        cd = gone // 2

        @pl.when((s == 2) & (gone >= 0) & (gone == 2 * cd) & (gone < 2 * n_b))
        def _():
            wait_recv(row(dx, cd), recv_dx.at[cd])
            remote(row(dx, cd), row(dx, cd), fwd.at[cd], recv_dx.at[cd], 3).start()

        @pl.when(is_f)
        def _():
            forward(k, c)

        @pl.when(~is_f)
        def _():
            backward(k, c)

        return 0

    lax.fori_loop(0, n_ops, step, 0)

    w1_copy(0, 0).wait()
    w1_copy(2, 1).wait()
    w2_copy(1, 0).wait()
    w2_copy(3, 1).wait()
    free_out(n_ops)
    free_out(n_ops + 1)
    if not n_f:
        half_blocks(_per_stage(s, EARLY))


def _scratch(nc, n_b, d, n_f):
    dma = pltpu.SemaphoreType.DMA
    sems = [dma((8,)), *[dma((2,))] * 13, *[dma((nc,))] * 5]
    return sems + [
        pltpu.VMEM((4, d, HT), BF16), pltpu.VMEM((4, HT, d), BF16),
        pltpu.VMEM((2, d, HT), BF16), pltpu.VMEM((2, HT, d), BF16),
        pltpu.VMEM((CH, d), F32), pltpu.VMEM((2, CH, d), BF16), pltpu.VMEM((2, CH, d), BF16),
        pltpu.VMEM((2, CH, HT), F32), pltpu.VMEM((2, CH, HT), F32),
        pltpu.VMEM((2, CH, HT), BF16), pltpu.VMEM((2, CH, HT), BF16)]


def _first_kernel(x, g, w1, w2, n_b):
    tokens, d = x.shape
    h = w1.shape[1]
    nc = tokens // CH
    rows = jax.ShapeDtypeStruct((tokens, d), BF16)
    wide = jax.ShapeDtypeStruct((tokens, h), BF16)
    anyspec = pl.BlockSpec(memory_space=pl.ANY)
    return pl.pallas_call(
        functools.partial(_pipe_kernel, nc, 0, n_b),
        out_shape=(rows, rows, rows, rows, wide, wide, jax.ShapeDtypeStruct((nc, h // HT, CH, HT), F32)),
        in_specs=[anyspec] * 4,
        out_specs=(anyspec,) * 7,
        scratch_shapes=_scratch(nc, n_b, d, nc),
        compiler_params=pltpu.CompilerParams(collective_id=0, has_side_effects=True, vmem_limit_bytes=VMEM_MAX),
        name='pipe_a',
    )(x, g, w1, w2)


def _second_kernel(g, w1, w2, gp, u, hin, y, dx, gin, dz, part, part1, b0):
    tokens, d = g.shape
    nc = tokens // CH
    n_b = nc - b0
    anyspec = pl.BlockSpec(memory_space=pl.ANY)
    both = (y, dx, gin, dz, part, part1)
    return pl.pallas_call(
        functools.partial(_pipe_kernel, 0, b0, n_b),
        out_shape=tuple(jax.ShapeDtypeStruct(a.shape, a.dtype) for a in both),
        in_specs=[anyspec] * 12,
        out_specs=(anyspec,) * len(both),
        scratch_shapes=_scratch(nc, n_b, d, 0),
        input_output_aliases={6 + i: i for i in range(len(both))},
        compiler_params=pltpu.CompilerParams(collective_id=1, has_side_effects=True, vmem_limit_bytes=VMEM_MAX),
        name='pipe_b',
    )(g, w1, w2, gp, u, hin, *both)


def _product(a_ref, b_ref, o_ref):
    o_ref[...] = _tn(a_ref[...], b_ref[...])


def _early_kernel(half, u, g, hin, dz, o, o1):
    n = _per_stage(lax.axis_index('stage'), EARLY)
    d = g.shape[1]
    n2, nd = u.shape[1] // HT, d // HT

    @pl.when(n > 0)
    def _():
        pltpu.emit_pipeline(
            _product, grid=(jnp.minimum(n, n2),),
            in_specs=[pl.BlockSpec((half, HT), lambda i: (0, i)), pl.BlockSpec((half, d), lambda i: (0, 0))],
            out_specs=[pl.BlockSpec((HT, d), lambda i: (i, 0))])(u, g, o)

    @pl.when(n > n2)
    def _():
        pltpu.emit_pipeline(
            _product, grid=(n - n2,),
            in_specs=[pl.BlockSpec((half, HT), lambda i: (0, lax.rem(i, nd))), pl.BlockSpec((half, d), lambda i: (0, lax.div(i, nd)))],
            out_specs=[pl.BlockSpec((HT, d), lambda i: (lax.rem(i, nd), lax.div(i, nd)))])(hin, dz, o1)


def _early(u, gin, hin, dz, half):
    h, d = u.shape[1], gin.shape[1]
    anyspec = pl.BlockSpec(memory_space=pl.ANY)
    return pl.pallas_call(
        functools.partial(_early_kernel, half),
        in_specs=[anyspec] * 4,
        out_specs=(anyspec,) * 2,
        out_shape=(jax.ShapeDtypeStruct((h, d), F32), jax.ShapeDtypeStruct((d, h), F32)),
        compiler_params=pltpu.CompilerParams(vmem_limit_bytes=VMEM_MAX),
        name='early',
    )(u, gin, hin, dz)


def _dw2_kernel(u_ref, g_ref, part_ref, y_ref, o_ref, yo_ref):
    yo_ref[...] = y_ref[...]
    o_ref[...] = part_ref[...] + _tn(u_ref[...], g_ref[...])


def _dw2(u, gin, part, y, half):
    tokens, h = u.shape
    d = gin.shape[1]
    steps = h // HT
    rows = pl.BlockSpec((tokens // steps, d), lambda i: (i, 0))
    blocks = pl.BlockSpec((HT, d), lambda i: (i, 0))
    return pl.pallas_call(
        _dw2_kernel,
        grid=(steps,),
        in_specs=[pl.BlockSpec((half, HT), lambda i: (1, i)),
                  pl.BlockSpec((half, d), lambda i: (1, 0), pipeline_mode=pl.Buffered(1)), blocks, rows],
        out_specs=(blocks, rows),
        out_shape=(jax.ShapeDtypeStruct((h, d), F32), jax.ShapeDtypeStruct(y.shape, BF16)),
        compiler_params=pltpu.CompilerParams(vmem_limit_bytes=VMEM_MAX, dimension_semantics=('arbitrary',)),
        name='dw2',
    )(u, gin, part, y)


def _dw1_late_kernel(h_ref, z_ref, part_ref, o_ref):
    o_ref[...] = part_ref[...] + _tn(h_ref[...], z_ref[...])


def _dw1_kernel(h_ref, z_ref, x_ref, _, o_ref, xo_ref):
    xo_ref[...] = x_ref[...]
    o_ref[...] = _tn(h_ref[...], z_ref[...])


def _dw1(hin, dz, part1, dx, half):
    tokens, d = hin.shape
    h = dz.shape[1]
    nd = d // HT
    blocks = pl.BlockSpec((HT, d), lambda i: (lax.rem(i, nd), lax.div(i, nd)))
    out = jax.ShapeDtypeStruct((d, h), F32)
    done = pl.pallas_call(
        _dw1_late_kernel,
        grid=(DW1_EARLY,),
        in_specs=[pl.BlockSpec((half, HT), lambda i: (1, lax.rem(i, nd))), pl.BlockSpec((half, d), lambda i: (1, lax.div(i, nd))), blocks],
        out_specs=blocks,
        out_shape=out,
        compiler_params=pltpu.CompilerParams(vmem_limit_bytes=VMEM_MAX, dimension_semantics=('arbitrary',)),
        name='dw1_late',
    )(hin, dz, part1)
    nj = h // HT - DW1_EARLY
    j0 = DW1_EARLY
    rows = pl.BlockSpec((tokens // (nj * nd), d), lambda i, j: (i * nj + j, 0))
    return pl.pallas_call(
        _dw1_kernel,
        grid=(nd, nj),
        in_specs=[pl.BlockSpec((tokens, HT), lambda i, j: (0, i)), pl.BlockSpec((tokens, HT), lambda i, j: (0, j0 + j)), rows,
                  pl.BlockSpec(memory_space=pl.ANY)],
        out_specs=(pl.BlockSpec((HT, HT), lambda i, j: (i, j0 + j)), rows),
        out_shape=(out, jax.ShapeDtypeStruct(dx.shape, BF16)),
        input_output_aliases={3: 0},
        compiler_params=pltpu.CompilerParams(vmem_limit_bytes=VMEM_MAX, dimension_semantics=('arbitrary', 'arbitrary')),
        name='dw1',
    )(hin, dz, dx, done)


def solution(mesh):
    def body(x, g, w1, w2):
        n_mb, mb, d = x.shape
        tokens = n_mb * mb
        b0 = tokens // CH // 2
        xt, gt = x.reshape(tokens, d), g.reshape(tokens, d)
        y, dx, hin, gin, u, dz, gp = _first_kernel(xt, gt, w1[0], w2[0], b0)
        half = tokens // 2
        part, part1 = _early(u, gin, hin, dz, half)
        y, dx, gin, dz, part, part1 = _second_kernel(gt, w1[0], w2[0], gp, u, hin, y, dx, gin, dz, part, part1, b0)
        dw2, y = _dw2(u, gin, part, y, half)
        dw1, dx = _dw1(hin, dz, part1, dx, half)
        return y.reshape(x.shape), dx.reshape(x.shape), dw1[None], dw2[None]

    return jax.shard_map(body, mesh=mesh,
                         in_specs=(P('data'), P('data'), P('stage'), P('stage')),
                         out_specs=(P('data'), P('data'), P(('data', 'stage')), P(('data', 'stage'))),
                         check_vma=False)
```
